32 devices in a mesh: lat: 8 (over y, x, core), lon: 4 (over z).
Axes of the slice: x: 2, y: 2, z: 4, core: 2. Of those that a mesh axis runs over, the one named last changes fastest.
Arguments:
- tokens: bfloat16 [2, 48, 96, 512], P(None, 'lat', 'lon'), may hold values from -6 to 6
- land_sea: int32 [48, 96], P('lat', 'lon'), may hold values 0 or 1
- land_vector: float32 [512], replicated, may hold values from -3 to 3
- fine_inward: bfloat16 [512, 768], replicated, may hold values from -0.25 to 0.25
- fine_outward: bfloat16 [256, 512], replicated, may hold values from -0.375 to 0.375
- fine_gain: float32 [512], replicated, may hold values from 0.25 to 1.75
- fine_scale: float32 [4], replicated, may hold values from 3 to 12
- merge_gain: float32 [2048], replicated, may hold values from 0.25 to 1.75
- merge_weight: bfloat16 [2048, 1024], replicated, may hold values from -0.125 to 0.125
- coarse_inward: bfloat16 [1024, 1536], replicated, may hold values from -0.1875 to 0.1875
- coarse_outward: bfloat16 [512, 1024], replicated, may hold values from -0.25 to 0.25
- coarse_gain: float32 [1024], replicated, may hold values from 0.25 to 1.75
- coarse_scale: float32 [8], replicated, may hold values from 3 to 12
- coarse_cotangent: bfloat16 [2, 24, 48, 1024], P(None, 'lat', 'lon'), may hold values from -6 to 6
Outputs:
- coarse_output: bfloat16 [2, 24, 48, 1024], P(None, 'lat', 'lon')
- token_grad: bfloat16 [2, 48, 96, 512], P(None, 'lat', 'lon')
The draws below stay inside these ranges and needn't reach their ends.
All inputs are finite; a program needn't handle non-finite values. No bound on the sum of `land_sea` on one device may be relied on, other than what follows from the above.
Results may differ from the reference program's by a relative error of at most 0.02.
Values may be sent and summed in bfloat16 or wider, within the bound.
No kernel may reach another device: no remote copies, remote signals or barrier semaphores. Data moves between devices by JAX's collectives and lax.ppermute only.
A program may use at most 64 MiB of HBM per device.

```python
import math
import jax
import jax.numpy as jnp
from jax import lax

D = 512
D2 = 1024
HEADS = 4
HEADS2 = 8
HD = 64
LEV = 2
WIN_LAT = 6
WIN_LON = 12
NLAT = 48
NLON = 96


def set_ends(entries, own_key, smallest, largest):
    extent = entries.shape
    index_at = [jax.random.randint(jax.random.fold_in(own_key, axis), (), 0, extent[axis]) for axis in range(len(extent))]
    entries = entries.at[tuple(index_at)].set(smallest)
    longest = extent.index(max(extent))
    index_at[longest] = (index_at[longest] + 1) % extent[longest]
    return entries.at[tuple(index_at)].set(largest)


def block_scale(rng, dims, split, low, top_value):
    level = 1.0
    for position, parts in split:
        heights = jax.random.uniform(jax.random.fold_in(jax.random.fold_in(rng, 6), position), (parts,), jnp.float32, low / len(split), top_value / len(split))
        level = level * jnp.repeat(jnp.exp(heights), dims[position] // parts).reshape((-1,) + (1,) * (len(dims) - 1 - position))
    return level


def bell_draw(own_key, extent, scale, limit, shards=(), kind=jnp.bfloat16):
    level = block_scale(own_key, extent, shards, -0.22, 0.18) if shards else 1.0
    result = jax.random.normal(own_key, extent, jnp.float32) * scale * level
    return jnp.minimum(jnp.maximum(result, -limit), limit).astype(kind)


def setup_inputs(seed: int = 0) -> dict:
    arg_keys = jax.random.split(jax.random.key(seed), 15)
    tokens = bell_draw(arg_keys[0], (LEV, NLAT, NLON, D), 1.0, 6.0, ((1, 8), (2, 4)))
    land_sea = set_ends((jax.random.randint(arg_keys[1], (NLAT, NLON), 0, 3) < 1).astype(jnp.int32), jax.random.fold_in(arg_keys[1], 1), 0, 1)
    land_vector = bell_draw(arg_keys[2], (D,), 0.5, 3.0, (), jnp.float32)
    fine_inward = bell_draw(arg_keys[3], (D, 3 * HEADS * HD), D ** -0.5, 0.25)
    fine_outward = bell_draw(arg_keys[4], (HEADS * HD, D), (HEADS * HD) ** -0.5, 0.375)
    fine_gain = jnp.clip(1.0 + 0.15 * jax.random.normal(arg_keys[5], (D,), jnp.float32), 0.25, 1.75)
    fine_scale = jnp.clip(jnp.exp(jax.random.uniform(arg_keys[6], (HEADS,), jnp.float32, math.log(3.0), math.log(12.0))), 3.0, 12.0)
    merge_gain = jnp.clip(1.0 + 0.15 * jax.random.normal(arg_keys[7], (4 * D,), jnp.float32), 0.25, 1.75)
    merge_weight = bell_draw(arg_keys[8], (4 * D, D2), (4 * D) ** -0.5, 0.125)
    coarse_inward = bell_draw(arg_keys[9], (D2, 3 * HEADS2 * HD), D2 ** -0.5, 0.1875)
    coarse_outward = bell_draw(arg_keys[10], (HEADS2 * HD, D2), (HEADS2 * HD) ** -0.5, 0.25)
    coarse_gain = jnp.clip(1.0 + 0.15 * jax.random.normal(arg_keys[11], (D2,), jnp.float32), 0.25, 1.75)
    coarse_scale = jnp.clip(jnp.exp(jax.random.uniform(arg_keys[12], (HEADS2,), jnp.float32, math.log(3.0), math.log(12.0))), 3.0, 12.0)
    coarse_cotangent = bell_draw(arg_keys[13], (LEV, NLAT // 2, NLON // 2, D2), 1.0, 6.0, ((1, 8), (2, 4)))
    return {"tokens": tokens, "land_sea": land_sea, "land_vector": land_vector, "fine_inward": fine_inward, "fine_outward": fine_outward, "fine_gain": fine_gain, "fine_scale": fine_scale, "merge_gain": merge_gain, "merge_weight": merge_weight, "coarse_inward": coarse_inward, "coarse_outward": coarse_outward, "coarse_gain": coarse_gain, "coarse_scale": coarse_scale, "coarse_cotangent": coarse_cotangent}


EPS_NORM = 1e-05
EPS_HEAD = 1e-06

def layer_norm(values, norm_gain):
    average = lax.optimization_barrier(jnp.mean(values, axis=-1, keepdims=True))
    centred = values - average
    spread = lax.optimization_barrier(jnp.mean(centred * centred, axis=-1, keepdims=True))
    return centred * lax.rsqrt(spread + EPS_NORM) * norm_gain

def into_windows(field):
    levels, height, breadth, channels = field.shape
    blocks = field.reshape(levels, height // WIN_LAT, WIN_LAT, breadth // WIN_LON, WIN_LON, channels)
    blocks = blocks.transpose(1, 3, 0, 2, 4, 5)
    return blocks.reshape(-1, levels * WIN_LAT * WIN_LON, channels)

def from_windows(blocks, levels, height, breadth):
    channels = blocks.shape[-1]
    field = blocks.reshape(height // WIN_LAT, breadth // WIN_LON, levels, WIN_LAT, WIN_LON, channels)
    return field.transpose(2, 0, 3, 1, 4, 5).reshape(levels, height, breadth, channels)

def attend(packed, scales, head_count, allowed):
    windows, length, width = packed.shape
    head_size = width // (3 * head_count)
    pieces = packed.reshape(windows, length, 3, head_count, head_size)
    queries = pieces[:, :, 0].astype(jnp.float32)
    key_rows = pieces[:, :, 1].astype(jnp.float32)
    values = pieces[:, :, 2]
    query_unit = (queries * lax.rsqrt(lax.optimization_barrier(jnp.mean(queries * queries, axis=-1, keepdims=True)) + EPS_HEAD)).astype(jnp.bfloat16)
    key_unit = (key_rows * lax.rsqrt(lax.optimization_barrier(jnp.mean(key_rows * key_rows, axis=-1, keepdims=True)) + EPS_HEAD)).astype(jnp.bfloat16)
    logits = jnp.einsum('wqhd,wkhd->whqk', query_unit.astype(jnp.float32), key_unit.astype(jnp.float32))
    logits = logits * (scales / head_size)[None, :, None, None]
    weights = jnp.exp(logits)
    if allowed is not None:
        weights = weights * allowed[:, None, :, :]
    attention = (weights / lax.optimization_barrier(jnp.sum(weights, axis=-1, keepdims=True))).astype(jnp.bfloat16)
    mixture = jnp.einsum('whqk,wkhd->wqhd', attention.astype(jnp.float32), values.astype(jnp.float32))
    return mixture.reshape(windows, length, head_count * head_size).astype(jnp.bfloat16)

def window_branch(packed, region, scales, outward, norm_gain, head_count):
    levels, height, breadth = (packed.shape[0], packed.shape[1], packed.shape[2])
    blocks = into_windows(packed)
    allowed = None
    if region is not None:
        marks = into_windows(region[..., None])[..., 0]
        allowed = (marks[:, :, None] == marks[:, None, :]).astype(jnp.float32)
    mixture = attend(blocks, scales, head_count, allowed)
    mixture = from_windows(mixture, levels, height, breadth)
    projected = jnp.dot(mixture, outward, preferred_element_type=jnp.float32)
    return layer_norm(projected, norm_gain)

def merge_patches(fine_field, norm_gain, weight):
    levels, height, breadth, channels = fine_field.shape
    grouped = fine_field.reshape(levels, height // 2, 2, breadth // 2, 2, channels)
    grouped = grouped.transpose(0, 1, 3, 4, 2, 5).reshape(levels, height // 2, breadth // 2, 4 * channels)
    normed = layer_norm(grouped.astype(jnp.float32), norm_gain).astype(jnp.bfloat16)
    return jnp.dot(normed, weight, preferred_element_type=jnp.float32).astype(jnp.bfloat16)

def reference(tokens, land_sea, land_vector, fine_inward, fine_outward, fine_gain, fine_scale, merge_gain, merge_weight, coarse_inward, coarse_outward, coarse_gain, coarse_scale, coarse_cotangent):
    half_lat = WIN_LAT // 2
    half_lon = WIN_LON // 2

    def fine_row(pieces):
        packed_row, band = pieces
        upper = ((jnp.arange(WIN_LAT, dtype=jnp.int32) < half_lat) & (band == 0)).astype(jnp.float32)
        region = jnp.broadcast_to(upper[None, :, None], (packed_row.shape[0], WIN_LAT, packed_row.shape[2]))
        return window_branch(packed_row, region, fine_scale, fine_outward, fine_gain, HEADS)

    def coarse_row(packed_row):
        return window_branch(packed_row, None, coarse_scale, coarse_outward, coarse_gain, HEADS2)

    def forward(token_field):
        biased = (token_field.astype(jnp.float32) + land_sea.astype(jnp.float32)[None, :, :, None] * land_vector).astype(jnp.bfloat16)
        levels, height, breadth, channels = biased.shape
        shifted = jnp.roll(biased, (half_lat, half_lon), axis=(1, 2))
        packed = jnp.dot(shifted, fine_inward, preferred_element_type=jnp.float32).astype(jnp.bfloat16)
        band_count = height // WIN_LAT
        packed_rows = packed.reshape(levels, band_count, WIN_LAT, breadth, packed.shape[-1]).transpose(1, 0, 2, 3, 4)
        band_ids = jnp.arange(band_count, dtype=jnp.int32)
        branch_rows = lax.map(jax.checkpoint(fine_row), (packed_rows, band_ids))
        branch = branch_rows.transpose(1, 0, 2, 3, 4).reshape(levels, height, breadth, channels)
        branch = jnp.roll(branch, (-half_lat, -half_lon), axis=(1, 2))
        fine_result = (biased.astype(jnp.float32) + branch).astype(jnp.bfloat16)
        coarse = merge_patches(fine_result, merge_gain, merge_weight)
        coarse_height, coarse_breadth, coarse_width = (coarse.shape[1], coarse.shape[2], coarse.shape[3])
        coarse_packed = jnp.dot(coarse, coarse_inward, preferred_element_type=jnp.float32).astype(jnp.bfloat16)
        coarse_bands = coarse_height // WIN_LAT
        coarse_rows = coarse_packed.reshape(levels, coarse_bands, WIN_LAT, coarse_breadth, coarse_packed.shape[-1]).transpose(1, 0, 2, 3, 4)
        coarse_branch = lax.map(jax.checkpoint(coarse_row), coarse_rows)
        coarse_branch = coarse_branch.transpose(1, 0, 2, 3, 4).reshape(levels, coarse_height, coarse_breadth, coarse_width)
        return (coarse.astype(jnp.float32) + coarse_branch).astype(jnp.bfloat16)
    coarse_output, pullback = jax.vjp(forward, tokens)
    token_grad, = pullback(coarse_cotangent)
    return (coarse_output, token_grad)
```

```python
import functools

import jax
import jax.numpy as jnp
import numpy as np
from jax import lax
from jax.experimental import pallas as pl
from jax.experimental.pallas import tpu as pltpu
from jax.sharding import PartitionSpec as P

HEADS = 4
HEADS2 = 8
WIN_LAT = 6
WIN_LON = 12

EPS_NORM = 1e-05
EPS_HEAD = 1e-06

F32 = jnp.float32
BF16 = jnp.bfloat16


def shifted_to(x, by_lat, by_lon):
    lats, lons = lax.axis_size("lat"), lax.axis_size("lon")
    pairs = [
        (i * lons + j, ((i + by_lat) % lats) * lons + (j + by_lon) % lons)
        for i in range(lats)
        for j in range(lons)
    ]
    return lax.ppermute(x, ("lat", "lon"), pairs)


def swapped(x):
    return lax.ppermute(x, "lat", [(i, i ^ 1) for i in range(lax.axis_size("lat"))])


def up8(n):
    return -(-n // 8) * 8


class Plan:
    def __init__(self, levels, height, breadth):
        half_lat, half_lon = WIN_LAT // 2, WIN_LON // 2
        assert height == WIN_LAT and breadth % WIN_LON == 0
        self.levels, self.height, self.breadth = levels, height, breadth
        self.cells = levels * height * breadth
        windows = breadth // WIN_LON
        cols = [(0, half_lon)]
        for w in range(1, windows):
            cols.append((half_lon + (w - 1) * WIN_LON, half_lon + w * WIN_LON))
        edge = [(breadth - half_lon, breadth)]

        def piece(first_row, ranges):
            rows, spans = [], []
            for low, high in ranges:
                cells = [
                    (l * height + r) * breadth + c
                    for l in range(levels)
                    for r in range(first_row, first_row + half_lat)
                    for c in range(low, high)
                ]
                spans.append((len(rows), up8(len(cells)), len(cells)))
                rows += cells + [-1] * (up8(len(cells)) - len(cells))
            return rows, spans

        a_rows, self.a_spans = piece(0, cols)
        b_rows, _ = piece(half_lat, cols)
        c_rows, self.c_spans = piece(0, edge)
        d_rows, _ = piece(half_lat, edge)
        self.sizes = [len(a_rows), len(b_rows), len(c_rows), len(d_rows)]
        order = np.array(a_rows + b_rows + c_rows + d_rows)
        self.rows = len(order)
        self.pack = (order[:, None] == np.arange(self.cells)[None, :]).astype(np.float32)
        half_h, half_b = height // 2, breadth // 2
        group = [
            (l * height + 2 * r + i) * breadth + 2 * c + j
            for j in range(2)
            for i in range(2)
            for l in range(levels)
            for r in range(half_h)
            for c in range(half_b)
        ]
        natural = (np.array(group)[:, None] == np.arange(self.cells)[None, :]).astype(np.float32)
        self.group = natural @ self.pack.T
        self.merged = levels * half_h * half_b
        self.masks = []
        for w in range(windows):
            size, real = self.a_spans[w][1], self.a_spans[w][2]
            block = np.where(np.arange(size) < real, 0, 2)
            upper = np.where(np.arange(size) < real, 1, 2)
            marks = [block, upper] + ([block, upper] if w == 0 else [])
            marks = np.concatenate(marks)
            flat = np.minimum(marks, 1) * (marks == 2)
            apart = (marks[:, None] == marks[None, :]).astype(np.float32)
            whole = (flat[:, None] == flat[None, :]).astype(np.float32)
            self.masks.append(np.stack([apart, whole]))

    def into_windows(self, a, b, c, d):
        result = []
        for w, (start, size, _) in enumerate(self.a_spans):
            parts = [a[start : start + size], b[start : start + size]]
            if w == 0:
                parts += [c, d]
            result.append(jnp.concatenate(parts, axis=0))
        return result

    def from_windows(self, windows):
        a, b = [], []
        for w, (_, size, _) in enumerate(self.a_spans):
            a.append(windows[w][:size])
            b.append(windows[w][size : 2 * size])
        base = 2 * self.a_spans[0][1]
        edge = self.c_spans[0][1]
        c = windows[0][base : base + edge]
        d = windows[0][base + edge :]
        return jnp.concatenate(a, axis=0), jnp.concatenate(b, axis=0), c, d


def mm(a, b):
    return lax.dot_general(a, b, (((1,), (0,)), ((), ())), preferred_element_type=F32)


def mm_t(a, b):
    return lax.dot_general(a, b, (((1,), (1,)), ((), ())), preferred_element_type=F32)


def t_mm(a, b):
    return lax.dot_general(a, b, (((0,), (0,)), ((), ())), preferred_element_type=F32)


def norm_parts(values):
    average = jnp.mean(values, axis=-1, keepdims=True)
    centred = values - average
    spread = jnp.mean(centred * centred, axis=-1, keepdims=True)
    factor = lax.rsqrt(spread + EPS_NORM)
    return centred * factor, factor


def norm_back(unit, factor, grad):
    first = jnp.mean(grad, axis=-1, keepdims=True)
    second = jnp.mean(grad * unit, axis=-1, keepdims=True)
    return factor * (grad - first - unit * second)


def head_lanes(lanes, size, index):
    lane = lax.broadcasted_iota(jnp.int32, (1, lanes), 1)
    return (lane >= index * size) & (lane < (index + 1) * size)


def head_mean_matrix(lanes, size):
    row = lax.broadcasted_iota(jnp.int32, (lanes, lanes), 0)
    col = lax.broadcasted_iota(jnp.int32, (lanes, lanes), 1)
    same = jnp.zeros((lanes, lanes), F32)
    for h in range(lanes // size):
        inside = (row >= h * size) & (row < (h + 1) * size) & (col >= h * size) & (col < (h + 1) * size)
        same = jnp.where(inside, 1.0 / size, same)
    return same.astype(BF16)


def unit_rows(rows, mean_matrix):
    squares = mm((rows * rows).astype(BF16), mean_matrix)
    factor = lax.rsqrt(squares + EPS_HEAD)
    return rows * factor, factor


def unit_back(unit, factor, grad, mean_matrix):
    overlap = mm((unit * grad).astype(BF16), mean_matrix)
    return factor * (grad - unit * overlap)


def spread_heads(rows, masks):
    return jnp.concatenate([jnp.where(m, rows, 0.0) for m in masks], axis=0).astype(BF16)


def join_heads(stacked, masks):
    n = stacked.shape[0] // len(masks)
    total = jnp.where(masks[0], stacked[:n], 0.0)
    for h in range(1, len(masks)):
        total = jnp.where(masks[h], stacked[h * n : (h + 1) * n], total)
    return total


def attend(query_stack, key_unit, values, masks, allowed):
    weights = jnp.exp(mm_t(query_stack, key_unit))
    if allowed is not None:
        weights = weights * jnp.concatenate([allowed] * len(masks), axis=0)
    totals = jnp.sum(weights, axis=-1, keepdims=True)
    probs = weights * (1.0 / totals)
    return probs


def attend_back(probs, query_stack, key_unit, values, mixture_grad, masks):
    grad_stack = spread_heads(mixture_grad, masks)
    probs_grad = mm_t(grad_stack, values)
    delta = jnp.sum(probs * probs_grad, axis=-1, keepdims=True)
    logits_grad = (probs * (probs_grad - delta)).astype(BF16)
    query_grad = join_heads(mm(logits_grad, key_unit), masks)
    key_grad = t_mm(logits_grad, query_stack)
    value_grad = t_mm(probs.astype(BF16), grad_stack)
    return query_grad, key_grad, value_grad


def bias_kernel(plan, tokens, land_sea, land_vector, pack, *outs):
    land = land_sea[...].astype(F32)
    breadth = plan.breadth
    eye = lax.broadcasted_iota(jnp.int32, (breadth, breadth), 0) == lax.broadcasted_iota(
        jnp.int32, (breadth, breadth), 1
    )
    vector = land_vector[...]
    rows = []
    for r in range(plan.height):
        column = jnp.sum(jnp.where(eye, land[r : r + 1, :], 0.0), axis=1, keepdims=True)
        rows.append(column * vector)
    biased = jnp.concatenate(
        [tokens[l, r].astype(F32) + rows[r] for l in range(plan.levels) for r in range(plan.height)],
        axis=0,
    ).astype(BF16)
    packed = mm(pack[...], biased)
    start = 0
    for out in outs:
        out[...] = packed[start : start + out.shape[0]].astype(BF16)
        start += out.shape[0]


def allowed_of(mask, first_band):
    return jnp.where(first_band, mask[0], mask[1])


def fine_window(rows, allowed, inward, outward, scale_lanes, masks, mean_matrix):
    inner = scale_lanes.shape[-1]
    packed = mm(rows.astype(BF16), inward).astype(BF16).astype(F32)
    query_unit, query_factor = unit_rows(packed[:, :inner], mean_matrix)
    key_unit, key_factor = unit_rows(packed[:, inner : 2 * inner], mean_matrix)
    values = packed[:, 2 * inner :].astype(BF16)
    query_stack = spread_heads(query_unit * scale_lanes, masks)
    probs = attend(query_stack, key_unit.astype(BF16), values, masks, allowed)
    mixture = join_heads(mm(probs.astype(BF16), values), masks).astype(BF16)
    unit, factor = norm_parts(mm(mixture, outward))
    return query_unit, query_factor, key_unit, key_factor, values, query_stack, probs, unit, factor


def scale_lanes_of(scales, masks, head_size):
    lanes = jnp.zeros(masks[0].shape, F32)
    for h, mask in enumerate(masks):
        lanes = jnp.where(mask, scales[h] / head_size, lanes)
    return lanes


def fine_setup(scales, inner):
    head_size = inner // HEADS
    masks = [head_lanes(inner, head_size, h) for h in range(HEADS)]
    return masks, scale_lanes_of(scales, masks, head_size), head_mean_matrix(inner, head_size)


def fine_kernel(plan, band, scales, a, b, c, d, inward, outward, gain, *rest):
    mask_refs, outs = rest[: len(plan.masks)], rest[len(plan.masks) :]
    masks, scale_lanes, mean_matrix = fine_setup(scales, outward.shape[0])
    first_band = band[0] == 0
    windows = plan.into_windows(*(x[...].astype(F32) for x in (a, b, c, d)))
    results = []
    for rows, mask in zip(windows, mask_refs):
        allowed = allowed_of(mask, first_band)
        unit = fine_window(
            rows, allowed, inward[...], outward[...], scale_lanes, masks, mean_matrix
        )[-2]
        results.append(rows + unit * gain[...])
    for out, value in zip(outs, plan.from_windows(results)):
        out[...] = value.astype(BF16)


def fine_back_kernel(plan, band, scales, a, b, c, d, ga, gb, gc, gd, inward, outward, gain, *rest):
    mask_refs, outs = rest[: len(plan.masks)], rest[len(plan.masks) :]
    masks, scale_lanes, mean_matrix = fine_setup(scales, outward.shape[0])
    first_band = band[0] == 0
    windows = plan.into_windows(*(x[...].astype(F32) for x in (a, b, c, d)))
    grads = plan.into_windows(*(x[...].astype(F32) for x in (ga, gb, gc, gd)))
    results = []
    for rows, grad, mask in zip(windows, grads, mask_refs):
        allowed = allowed_of(mask, first_band)
        query_unit, query_factor, key_unit, key_factor, values, query_stack, probs, unit, factor = (
            fine_window(rows, allowed, inward[...], outward[...], scale_lanes, masks, mean_matrix)
        )
        projected_grad = norm_back(unit, factor, grad * gain[...]).astype(BF16)
        mixture_grad = mm_t(projected_grad, outward[...])
        query_grad, key_grad, value_grad = attend_back(
            probs, query_stack, key_unit.astype(BF16), values, mixture_grad, masks
        )
        query_grad = unit_back(query_unit, query_factor, query_grad * scale_lanes, mean_matrix)
        key_grad = unit_back(key_unit, key_factor, key_grad, mean_matrix)
        packed_grad = jnp.concatenate(
            [query_grad.astype(BF16), key_grad.astype(BF16), value_grad.astype(BF16)], axis=1
        )
        results.append(grad + mm_t(packed_grad, inward[...]))
    for out, value in zip(outs, plan.from_windows(results)):
        out[...] = value.astype(BF16)


def merge_kernel(plan, a, b, c, d, group, gain, weight, coarse, grouped_out):
    pieces = jnp.concatenate([x[...].astype(F32) for x in (a, b, c, d)], axis=0).astype(BF16)
    rows = mm(group[...], pieces)
    n = plan.merged
    grouped = jnp.concatenate([rows[g * n : (g + 1) * n] for g in range(4)], axis=1)
    unit, _ = norm_parts(grouped)
    normed = (unit * gain[...]).astype(BF16)
    coarse[...] = mm(normed, weight[...]).astype(BF16)
    grouped_out[...] = grouped.astype(BF16)


def coarse_kernel(
    plan,
    scales,
    own,
    partner,
    own_cot,
    partner_cot,
    grouped,
    inward,
    outward,
    gain,
    merge_gain,
    merge_weight,
    ungroup,
    coarse_out,
    ga,
    gb,
    gc,
    gd,
    cot_rows,
    out_rows,
):
    inner = outward.shape[0]
    head_size = inner // HEADS2
    n = plan.merged
    half_b = plan.breadth // 2
    lines = [(l, r) for l in range(plan.levels) for r in range(plan.height // 2)]
    for k, (l, r) in enumerate(lines):
        cot_rows[k * half_b : (k + 1) * half_b, :] = own_cot[l, r].astype(F32)
        cot_rows[n + k * half_b : n + (k + 1) * half_b, :] = partner_cot[l, r].astype(F32)
    rows = jnp.concatenate([own[...].astype(F32), partner[...].astype(F32)], axis=0)
    packed = mm(rows.astype(BF16), inward[...]).astype(BF16).astype(F32)
    part = 256 if inner % 256 == 0 else inner
    per = part // head_size
    masks = [head_lanes(part, head_size, h) for h in range(per)]
    mean_matrix = head_mean_matrix(part, head_size)
    saved, mixtures = [], []
    for g in range(inner // part):
        low = g * part
        scale_lanes = scale_lanes_of([scales[g * per + h] for h in range(per)], masks, head_size)
        query_unit, query_factor = unit_rows(packed[:, low : low + part], mean_matrix)
        key_unit, key_factor = unit_rows(packed[:, inner + low : inner + low + part], mean_matrix)
        values = packed[:, 2 * inner + low : 2 * inner + low + part].astype(BF16)
        query_stack = spread_heads(query_unit * scale_lanes, masks)
        key_low = key_unit.astype(BF16)
        probs = attend(query_stack, key_low, values, masks, None)
        mixtures.append(join_heads(mm(probs.astype(BF16), values), masks).astype(BF16))
        saved.append(
            (query_unit, query_factor, key_unit, key_factor, values, query_stack, key_low, probs, scale_lanes)
        )
    unit, factor = norm_parts(mm(jnp.concatenate(mixtures, axis=1), outward[...]))
    out_rows[...] = rows[:n] + unit[:n] * gain[...]
    for k, (l, r) in enumerate(lines):
        coarse_out[l, r] = out_rows[k * half_b : (k + 1) * half_b, :].astype(BF16)

    cot = cot_rows[...]
    projected_grad = norm_back(unit, factor, cot * gain[...]).astype(BF16)
    mixture_grad = mm_t(projected_grad, outward[...])
    query_grads, key_grads, value_grads = [], [], []
    for g, (query_unit, query_factor, key_unit, key_factor, values, query_stack, key_low, probs, scale_lanes) in enumerate(saved):
        low = g * part
        query_grad, key_grad, value_grad = attend_back(
            probs, query_stack, key_low, values, mixture_grad[:, low : low + part], masks
        )
        query_grads.append(
            unit_back(query_unit[:n], query_factor[:n], query_grad[:n] * scale_lanes, mean_matrix).astype(BF16)
        )
        key_grads.append(unit_back(key_unit[:n], key_factor[:n], key_grad[:n], mean_matrix).astype(BF16))
        value_grads.append(value_grad[:n].astype(BF16))
    packed_grad = jnp.concatenate(query_grads + key_grads + value_grads, axis=1)
    coarse_grad = (cot[:n] + mm_t(packed_grad, inward[...])).astype(BF16)

    normed_grad = mm_t(coarse_grad, merge_weight[...])
    merge_unit, merge_factor = norm_parts(grouped[...].astype(F32))
    grouped_grad = norm_back(merge_unit, merge_factor, normed_grad * merge_gain[...])
    width = grouped_grad.shape[1] // 4
    stacked = jnp.concatenate(
        [grouped_grad[:, g * width : (g + 1) * width] for g in range(4)], axis=0
    ).astype(BF16)
    pieces = mm(ungroup[...], stacked)
    start = 0
    for out in (ga, gb, gc, gd):
        out[...] = pieces[start : start + out.shape[0]].astype(BF16)
        start += out.shape[0]


def unpack_kernel(plan, a, b, c, d, unpack, out):
    pieces = jnp.concatenate([x[...].astype(F32) for x in (a, b, c, d)], axis=0).astype(BF16)
    rows = mm(unpack[...], pieces)
    k = 0
    for l in range(plan.levels):
        for r in range(plan.height):
            out[l, r] = rows[k : k + plan.breadth].astype(BF16)
            k += plan.breadth


SMEM = functools.partial(pl.BlockSpec, memory_space=pltpu.SMEM)
VMEM = functools.partial(pl.BlockSpec, memory_space=pltpu.VMEM)


def call(kernel, name, outs, args, smem=0, scratch=()):
    specs = [SMEM()] * smem + [VMEM()] * (len(args) - smem)
    return pl.pallas_call(
        kernel,
        name=name,
        out_shape=outs,
        in_specs=specs,
        out_specs=[VMEM() for _ in outs],
        scratch_shapes=scratch,
        compiler_params=pltpu.CompilerParams(vmem_limit_bytes=56 * 1024 * 1024),
    )(*args)


def local(
    tokens,
    land_sea,
    land_vector,
    fine_inward,
    fine_outward,
    fine_gain,
    fine_scale,
    merge_gain,
    merge_weight,
    coarse_inward,
    coarse_outward,
    coarse_gain,
    coarse_scale,
    coarse_cotangent,
):
    levels, height, breadth, width = tokens.shape
    width2 = coarse_cotangent.shape[-1]
    plan = Plan(levels, height, breadth)
    pieces = [jax.ShapeDtypeStruct((n, width), BF16) for n in plan.sizes]
    constant = lambda x: jnp.asarray(x, BF16)
    row = lambda x: x.reshape(1, -1)
    band = lax.axis_index("lat").astype(jnp.int32).reshape(1)
    masks = [jnp.asarray(m, F32) for m in plan.masks]

    partner_cot = swapped(coarse_cotangent)

    def gather(a, b, c, d):
        return a, shifted_to(b, 1, 0), shifted_to(c, 0, 1), shifted_to(d, 1, 1)

    def give_back(a, b, c, d):
        return a, shifted_to(b, -1, 0), shifted_to(c, 0, -1), shifted_to(d, -1, -1)

    region = gather(
        *call(
            functools.partial(bias_kernel, plan),
            "bias",
            pieces,
            (tokens, land_sea, row(land_vector), constant(plan.pack)),
        )
    )
    fine_result = give_back(
        *call(
            functools.partial(fine_kernel, plan),
            "fine",
            pieces,
            (band, fine_scale, *region, fine_inward, fine_outward, row(fine_gain), *masks),
            smem=2,
        )
    )
    own, grouped = call(
        functools.partial(merge_kernel, plan),
        "merge",
        [
            jax.ShapeDtypeStruct((plan.merged, width2), BF16),
            jax.ShapeDtypeStruct((plan.merged, 4 * width), BF16),
        ],
        (*fine_result, constant(plan.group), row(merge_gain), merge_weight),
    )
    partner = swapped(own)
    coarse_output, *grads = call(
        functools.partial(coarse_kernel, plan),
        "coarse",
        [jax.ShapeDtypeStruct(coarse_cotangent.shape, BF16)] + pieces,
        (
            coarse_scale,
            own,
            partner,
            coarse_cotangent,
            partner_cot,
            grouped,
            coarse_inward,
            coarse_outward,
            row(coarse_gain),
            row(merge_gain),
            merge_weight,
            constant(plan.group.T),
        ),
        smem=1,
        scratch=[
            pltpu.VMEM((2 * plan.merged, width2), F32),
            pltpu.VMEM((plan.merged, width2), F32),
        ],
    )
    grads = gather(*grads)
    token_pieces = give_back(
        *call(
            functools.partial(fine_back_kernel, plan),
            "fine_back",
            pieces,
            (
                band,
                fine_scale,
                *region,
                *grads,
                fine_inward,
                fine_outward,
                row(fine_gain),
                *masks,
            ),
            smem=2,
        )
    )
    (token_grad,) = call(
        functools.partial(unpack_kernel, plan),
        "unpack",
        [jax.ShapeDtypeStruct(tokens.shape, BF16)],
        (*token_pieces, constant(plan.pack.T)),
    )
    return (coarse_output, token_grad)


def solution(mesh):
    whole, cells = P(), P(None, "lat", "lon", None)
    return jax.shard_map(
        local,
        mesh=mesh,
        in_specs=(cells, P("lat", "lon")) + (whole,) * 11 + (cells,),
        out_specs=(cells, cells),
        check_vma=False,
    )
```

```python
import functools

import jax
import jax.numpy as jnp
import numpy as np
from jax import lax
from jax.experimental import pallas as pl
from jax.experimental.pallas import tpu as pltpu
from jax.sharding import PartitionSpec as P

HEADS = 4
HEADS2 = 8
WIN_LAT = 6
WIN_LON = 12

EPS_NORM = 1e-05
EPS_HEAD = 1e-06

F32 = jnp.float32
BF16 = jnp.bfloat16


def shifted_to(x, by_lat, by_lon):
    lats, lons = lax.axis_size("lat"), lax.axis_size("lon")
    pairs = [
        (i * lons + j, ((i + by_lat) % lats) * lons + (j + by_lon) % lons)
        for i in range(lats)
        for j in range(lons)
    ]
    return lax.ppermute(x, ("lat", "lon"), pairs)


def swapped(x):
    return lax.ppermute(x, "lat", [(i, i ^ 1) for i in range(lax.axis_size("lat"))])


def up8(n):
    return -(-n // 8) * 8


class Plan:
    def __init__(self, levels, height, breadth):
        half_lat, half_lon = WIN_LAT // 2, WIN_LON // 2
        assert height == WIN_LAT and breadth % WIN_LON == 0
        self.levels, self.height, self.breadth = levels, height, breadth
        self.cells = levels * height * breadth
        windows = breadth // WIN_LON
        cols = [(0, half_lon)]
        for w in range(1, windows):
            cols.append((half_lon + (w - 1) * WIN_LON, half_lon + w * WIN_LON))
        edge = [(breadth - half_lon, breadth)]

        def piece(first_row, ranges):
            rows, spans = [], []
            for low, high in ranges:
                cells = [
                    (l * height + r) * breadth + c
                    for l in range(levels)
                    for r in range(first_row, first_row + half_lat)
                    for c in range(low, high)
                ]
                spans.append((len(rows), up8(len(cells)), len(cells)))
                rows += cells + [-1] * (up8(len(cells)) - len(cells))
            return rows, spans

        a_rows, self.a_spans = piece(0, cols)
        b_rows, _ = piece(half_lat, cols)
        c_rows, self.c_spans = piece(0, edge)
        d_rows, _ = piece(half_lat, edge)
        self.sizes = [len(a_rows), len(b_rows), len(c_rows), len(d_rows)]
        order = np.array(a_rows + b_rows + c_rows + d_rows)
        self.rows = len(order)
        self.pack = (order[:, None] == np.arange(self.cells)[None, :]).astype(np.float32)
        half_h, half_b = height // 2, breadth // 2
        group = [
            (l * height + 2 * r + i) * breadth + 2 * c + j
            for j in range(2)
            for i in range(2)
            for l in range(levels)
            for r in range(half_h)
            for c in range(half_b)
        ]
        natural = (np.array(group)[:, None] == np.arange(self.cells)[None, :]).astype(np.float32)
        self.group = natural @ self.pack.T
        self.merged = levels * half_h * half_b
        self.masks = []
        for w in range(windows):
            size, real = self.a_spans[w][1], self.a_spans[w][2]
            block = np.where(np.arange(size) < real, 0, 2)
            upper = np.where(np.arange(size) < real, 1, 2)
            marks = [block, upper] + ([block, upper] if w == 0 else [])
            marks = np.concatenate(marks)
            flat = np.minimum(marks, 1) * (marks == 2)
            apart = (marks[:, None] == marks[None, :]).astype(np.float32)
            whole = (flat[:, None] == flat[None, :]).astype(np.float32)
            self.masks.append(np.stack([apart, whole]))

    def into_windows(self, a, b, c, d):
        result = []
        for w, (start, size, _) in enumerate(self.a_spans):
            parts = [a[start : start + size], b[start : start + size]]
            if w == 0:
                parts += [c, d]
            result.append(jnp.concatenate(parts, axis=0))
        return result

    def from_windows(self, windows):
        a, b = [], []
        for w, (_, size, _) in enumerate(self.a_spans):
            a.append(windows[w][:size])
            b.append(windows[w][size : 2 * size])
        base = 2 * self.a_spans[0][1]
        edge = self.c_spans[0][1]
        c = windows[0][base : base + edge]
        d = windows[0][base + edge :]
        return jnp.concatenate(a, axis=0), jnp.concatenate(b, axis=0), c, d


def mm(a, b):
    return lax.dot_general(a, b, (((1,), (0,)), ((), ())), preferred_element_type=F32)


def mm_t(a, b):
    return lax.dot_general(a, b, (((1,), (1,)), ((), ())), preferred_element_type=F32)


def t_mm(a, b):
    return lax.dot_general(a, b, (((0,), (0,)), ((), ())), preferred_element_type=F32)


def norm_parts(values):
    average = jnp.mean(values, axis=-1, keepdims=True)
    centred = values - average
    spread = jnp.mean(centred * centred, axis=-1, keepdims=True)
    factor = lax.rsqrt(spread + EPS_NORM)
    return centred * factor, factor


def norm_back(unit, factor, grad):
    first = jnp.mean(grad, axis=-1, keepdims=True)
    second = jnp.mean(grad * unit, axis=-1, keepdims=True)
    return factor * (grad - first - unit * second)


def head_lanes(lanes, size, index):
    lane = lax.broadcasted_iota(jnp.int32, (1, lanes), 1)
    return (lane >= index * size) & (lane < (index + 1) * size)


def head_mean_matrix(lanes, size):
    row = lax.broadcasted_iota(jnp.int32, (lanes, lanes), 0)
    col = lax.broadcasted_iota(jnp.int32, (lanes, lanes), 1)
    same = jnp.zeros((lanes, lanes), F32)
    for h in range(lanes // size):
        inside = (row >= h * size) & (row < (h + 1) * size) & (col >= h * size) & (col < (h + 1) * size)
        same = jnp.where(inside, 1.0 / size, same)
    return same.astype(BF16)


def unit_rows(rows, mean_matrix):
    squares = mm((rows * rows).astype(BF16), mean_matrix)
    factor = lax.rsqrt(squares + EPS_HEAD)
    return rows * factor, factor


def unit_back(unit, factor, grad, mean_matrix):
    overlap = mm((unit * grad).astype(BF16), mean_matrix)
    return factor * (grad - unit * overlap)


def spread_heads(rows, masks):
    return jnp.concatenate([jnp.where(m, rows, 0.0) for m in masks], axis=0).astype(BF16)


def join_heads(stacked, masks):
    n = stacked.shape[0] // len(masks)
    total = jnp.where(masks[0], stacked[:n], 0.0)
    for h in range(1, len(masks)):
        total = jnp.where(masks[h], stacked[h * n : (h + 1) * n], total)
    return total


def attend(query_stack, key_unit, values, masks, allowed):
    weights = jnp.exp(mm_t(query_stack, key_unit))
    if allowed is not None:
        weights = weights * jnp.concatenate([allowed] * len(masks), axis=0)
    totals = jnp.sum(weights, axis=-1, keepdims=True)
    probs = weights * (1.0 / totals)
    return probs


def attend_back(probs, query_stack, key_unit, values, mixture_grad, masks):
    grad_stack = spread_heads(mixture_grad, masks)
    probs_grad = mm_t(grad_stack, values)
    delta = jnp.sum(probs * probs_grad, axis=-1, keepdims=True)
    logits_grad = (probs * (probs_grad - delta)).astype(BF16)
    query_grad = join_heads(mm(logits_grad, key_unit), masks)
    key_grad = t_mm(logits_grad, query_stack)
    value_grad = t_mm(probs.astype(BF16), grad_stack)
    return query_grad, key_grad, value_grad


def bias_kernel(plan, tokens, land_sea, land_vector, pack, *outs):
    land = land_sea[...].astype(F32)
    breadth = plan.breadth
    eye = lax.broadcasted_iota(jnp.int32, (breadth, breadth), 0) == lax.broadcasted_iota(
        jnp.int32, (breadth, breadth), 1
    )
    vector = land_vector[...]
    rows = []
    for r in range(plan.height):
        column = jnp.sum(jnp.where(eye, land[r : r + 1, :], 0.0), axis=1, keepdims=True)
        rows.append(column * vector)
    biased = jnp.concatenate(
        [tokens[l, r].astype(F32) + rows[r] for l in range(plan.levels) for r in range(plan.height)],
        axis=0,
    ).astype(BF16)
    packed = mm(pack[...], biased)
    start = 0
    for out in outs:
        out[...] = packed[start : start + out.shape[0]].astype(BF16)
        start += out.shape[0]


def allowed_of(mask, first_band):
    return jnp.where(first_band, mask[0], mask[1])


def fine_window(rows, allowed, inward, outward, scale_lanes, masks, mean_matrix):
    inner = scale_lanes.shape[-1]
    packed = mm(rows.astype(BF16), inward).astype(BF16).astype(F32)
    query_unit, query_factor = unit_rows(packed[:, :inner], mean_matrix)
    key_unit, key_factor = unit_rows(packed[:, inner : 2 * inner], mean_matrix)
    values = packed[:, 2 * inner :].astype(BF16)
    query_stack = spread_heads(query_unit * scale_lanes, masks)
    probs = attend(query_stack, key_unit.astype(BF16), values, masks, allowed)
    mixture = join_heads(mm(probs.astype(BF16), values), masks).astype(BF16)
    unit, factor = norm_parts(mm(mixture, outward))
    return query_unit, query_factor, key_unit, key_factor, values, query_stack, probs, unit, factor


def scale_lanes_of(scales, masks, head_size):
    lanes = jnp.zeros(masks[0].shape, F32)
    for h, mask in enumerate(masks):
        lanes = jnp.where(mask, scales[h] / head_size, lanes)
    return lanes


def fine_setup(scales, inner):
    head_size = inner // HEADS
    masks = [head_lanes(inner, head_size, h) for h in range(HEADS)]
    return masks, scale_lanes_of(scales, masks, head_size), head_mean_matrix(inner, head_size)


def fine_kernel(plan, band, scales, a, b, c, d, inward, outward, gain, *rest):
    mask_refs, outs = rest[: len(plan.masks)], rest[len(plan.masks) :]
    masks, scale_lanes, mean_matrix = fine_setup(scales, outward.shape[0])
    first_band = band[0] == 0
    windows = plan.into_windows(*(x[...].astype(F32) for x in (a, b, c, d)))
    results = []
    for rows, mask in zip(windows, mask_refs):
        allowed = allowed_of(mask, first_band)
        unit = fine_window(
            rows, allowed, inward[...], outward[...], scale_lanes, masks, mean_matrix
        )[-2]
        results.append(rows + unit * gain[...])
    for out, value in zip(outs, plan.from_windows(results)):
        out[...] = value.astype(BF16)


def fine_back_kernel(plan, band, scales, a, b, c, d, ga, gb, gc, gd, inward, outward, gain, *rest):
    mask_refs, outs = rest[: len(plan.masks)], rest[len(plan.masks) :]
    masks, scale_lanes, mean_matrix = fine_setup(scales, outward.shape[0])
    first_band = band[0] == 0
    windows = plan.into_windows(*(x[...].astype(F32) for x in (a, b, c, d)))
    grads = plan.into_windows(*(x[...].astype(F32) for x in (ga, gb, gc, gd)))
    results = []
    for rows, grad, mask in zip(windows, grads, mask_refs):
        allowed = allowed_of(mask, first_band)
        query_unit, query_factor, key_unit, key_factor, values, query_stack, probs, unit, factor = (
            fine_window(rows, allowed, inward[...], outward[...], scale_lanes, masks, mean_matrix)
        )
        projected_grad = norm_back(unit, factor, grad * gain[...]).astype(BF16)
        mixture_grad = mm_t(projected_grad, outward[...])
        query_grad, key_grad, value_grad = attend_back(
            probs, query_stack, key_unit.astype(BF16), values, mixture_grad, masks
        )
        query_grad = unit_back(query_unit, query_factor, query_grad * scale_lanes, mean_matrix)
        key_grad = unit_back(key_unit, key_factor, key_grad, mean_matrix)
        packed_grad = jnp.concatenate(
            [query_grad.astype(BF16), key_grad.astype(BF16), value_grad.astype(BF16)], axis=1
        )
        results.append(grad + mm_t(packed_grad, inward[...]))
    for out, value in zip(outs, plan.from_windows(results)):
        out[...] = value.astype(BF16)


def merge_kernel(plan, a, b, c, d, group, gain, weight, coarse, grouped_out):
    pieces = jnp.concatenate([x[...].astype(F32) for x in (a, b, c, d)], axis=0).astype(BF16)
    rows = mm(group[...], pieces)
    n = plan.merged
    grouped = jnp.concatenate([rows[g * n : (g + 1) * n] for g in range(4)], axis=1)
    unit, _ = norm_parts(grouped)
    normed = (unit * gain[...]).astype(BF16)
    coarse[...] = mm(normed, weight[...]).astype(BF16)
    grouped_out[...] = grouped.astype(BF16)


def coarse_kernel(
    plan,
    scales,
    own,
    partner,
    own_cot,
    partner_cot,
    grouped,
    inward,
    outward,
    gain,
    merge_gain,
    merge_weight,
    ungroup,
    coarse_out,
    ga,
    gb,
    gc,
    gd,
    cot_rows,
    out_rows,
):
    inner = outward.shape[0]
    head_size = inner // HEADS2
    n = plan.merged
    half_b = plan.breadth // 2
    lines = [(l, r) for l in range(plan.levels) for r in range(plan.height // 2)]
    for k, (l, r) in enumerate(lines):
        cot_rows[k * half_b : (k + 1) * half_b, :] = own_cot[l, r].astype(F32)
        cot_rows[n + k * half_b : n + (k + 1) * half_b, :] = partner_cot[l, r].astype(F32)
    rows = jnp.concatenate([own[...].astype(F32), partner[...].astype(F32)], axis=0)
    packed = mm(rows.astype(BF16), inward[...]).astype(BF16).astype(F32)
    part = 256 if inner % 256 == 0 else inner
    per = part // head_size
    masks = [head_lanes(part, head_size, h) for h in range(per)]
    mean_matrix = head_mean_matrix(part, head_size)
    saved, mixtures = [], []
    for g in range(inner // part):
        low = g * part
        scale_lanes = scale_lanes_of([scales[g * per + h] for h in range(per)], masks, head_size)
        query_unit, query_factor = unit_rows(packed[:, low : low + part], mean_matrix)
        key_unit, key_factor = unit_rows(packed[:, inner + low : inner + low + part], mean_matrix)
        values = packed[:, 2 * inner + low : 2 * inner + low + part].astype(BF16)
        query_stack = spread_heads(query_unit * scale_lanes, masks)
        key_low = key_unit.astype(BF16)
        probs = attend(query_stack, key_low, values, masks, None)
        mixtures.append(join_heads(mm(probs.astype(BF16), values), masks).astype(BF16))
        saved.append(
            (query_unit, query_factor, key_unit, key_factor, values, query_stack, key_low, probs, scale_lanes)
        )
    unit, factor = norm_parts(mm(jnp.concatenate(mixtures, axis=1), outward[...]))
    out_rows[...] = rows[:n] + unit[:n] * gain[...]
    for k, (l, r) in enumerate(lines):
        coarse_out[l, r] = out_rows[k * half_b : (k + 1) * half_b, :].astype(BF16)

    cot = cot_rows[...]
    projected_grad = norm_back(unit, factor, cot * gain[...]).astype(BF16)
    mixture_grad = mm_t(projected_grad, outward[...])
    query_grads, key_grads, value_grads = [], [], []
    for g, (query_unit, query_factor, key_unit, key_factor, values, query_stack, key_low, probs, scale_lanes) in enumerate(saved):
        low = g * part
        query_grad, key_grad, value_grad = attend_back(
            probs, query_stack, key_low, values, mixture_grad[:, low : low + part], masks
        )
        query_grads.append(
            unit_back(query_unit[:n], query_factor[:n], query_grad[:n] * scale_lanes, mean_matrix).astype(BF16)
        )
        key_grads.append(unit_back(key_unit[:n], key_factor[:n], key_grad[:n], mean_matrix).astype(BF16))
        value_grads.append(value_grad[:n].astype(BF16))
    packed_grad = jnp.concatenate(query_grads + key_grads + value_grads, axis=1)
    coarse_grad = (cot[:n] + mm_t(packed_grad, inward[...])).astype(BF16)

    normed_grad = mm_t(coarse_grad, merge_weight[...])
    merge_unit, merge_factor = norm_parts(grouped[...].astype(F32))
    grouped_grad = norm_back(merge_unit, merge_factor, normed_grad * merge_gain[...])
    width = grouped_grad.shape[1] // 4
    stacked = jnp.concatenate(
        [grouped_grad[:, g * width : (g + 1) * width] for g in range(4)], axis=0
    ).astype(BF16)
    pieces = mm(ungroup[...], stacked)
    start = 0
    for out in (ga, gb, gc, gd):
        out[...] = pieces[start : start + out.shape[0]].astype(BF16)
        start += out.shape[0]


def unpack_kernel(plan, a, b, c, d, unpack, out):
    pieces = jnp.concatenate([x[...].astype(F32) for x in (a, b, c, d)], axis=0).astype(BF16)
    rows = mm(unpack[...], pieces)
    k = 0
    for l in range(plan.levels):
        for r in range(plan.height):
            out[l, r] = rows[k : k + plan.breadth].astype(BF16)
            k += plan.breadth


SMEM = functools.partial(pl.BlockSpec, memory_space=pltpu.SMEM)
VMEM = functools.partial(pl.BlockSpec, memory_space=pltpu.VMEM)


def call(kernel, name, outs, args, smem=0, scratch=(), keep_in=True, keep_out=True):
    specs = [SMEM()] * smem + [VMEM()] * (len(args) - smem)
    space = pltpu.VMEM if keep_in else pltpu.HBM
    near = tuple(pltpu.with_memory_space_constraint(x, space) for x in args[smem:])
    args = tuple(args[:smem]) + near
    if keep_out:
        outs = [pltpu.VMEM(o.shape, o.dtype) for o in outs]
    return pl.pallas_call(
        kernel,
        name=name,
        out_shape=outs,
        in_specs=specs,
        out_specs=[VMEM() for _ in outs],
        scratch_shapes=scratch,
        compiler_params=pltpu.CompilerParams(vmem_limit_bytes=24 * 1024 * 1024),
    )(*args)


def load_kernel(after, *refs):
    n = (len(refs) - 1) // 2
    sems = refs[-1]
    copies = [pltpu.make_async_copy(refs[k], refs[n + k], sems.at[k]) for k in range(n)]
    for copy in copies:
        copy.start()
    for copy in copies:
        copy.wait()


def load(after, args):
    anywhere = pl.BlockSpec(memory_space=pl.ANY)
    args = tuple(pltpu.with_memory_space_constraint(x, pltpu.HBM) for x in args)
    return pl.pallas_call(
        load_kernel,
        name="load",
        out_shape=[pltpu.VMEM(x.shape, x.dtype) for x in args],
        in_specs=[anywhere] * (len(args) + 1),
        out_specs=[VMEM() for _ in args],
        scratch_shapes=[pltpu.SemaphoreType.DMA((len(args),))],
        compiler_params=pltpu.CompilerParams(vmem_limit_bytes=24 * 1024 * 1024),
    )(after, *args)


def local(
    tokens,
    land_sea,
    land_vector,
    fine_inward,
    fine_outward,
    fine_gain,
    fine_scale,
    merge_gain,
    merge_weight,
    coarse_inward,
    coarse_outward,
    coarse_gain,
    coarse_scale,
    coarse_cotangent,
):
    levels, height, breadth, width = tokens.shape
    width2 = coarse_cotangent.shape[-1]
    plan = Plan(levels, height, breadth)
    pieces = [jax.ShapeDtypeStruct((n, width), BF16) for n in plan.sizes]
    constant = lambda x: jnp.asarray(x, BF16)
    row = lambda x: x.reshape(1, -1)
    band = lax.axis_index("lat").astype(jnp.int32).reshape(1)
    masks = [jnp.asarray(m, F32) for m in plan.masks]

    def gather(a, b, c, d):
        return a, shifted_to(b, 1, 0), shifted_to(c, 0, 1), shifted_to(d, 1, 1)

    def give_back(a, b, c, d):
        return a, shifted_to(b, -1, 0), shifted_to(c, 0, -1), shifted_to(d, -1, -1)

    biased = call(
        functools.partial(bias_kernel, plan),
        "bias",
        pieces,
        (tokens, land_sea, row(land_vector), constant(plan.pack)),
        keep_in=False,
    )
    region = gather(*biased)
    (
        fine_inward,
        fine_outward,
        merge_weight,
        coarse_inward,
        coarse_outward,
        fine_gain,
        merge_gain,
        coarse_gain,
        group,
        ungroup,
        unpack,
        *masks,
    ) = load(
        biased[0],
        (
            fine_inward,
            fine_outward,
            merge_weight,
            coarse_inward,
            coarse_outward,
            row(fine_gain),
            row(merge_gain),
            row(coarse_gain),
            constant(plan.group),
            constant(plan.group.T),
            constant(plan.pack.T),
            *masks,
        ),
    )
    fine_weights = (fine_inward, fine_outward, fine_gain, *masks)
    fine_result = give_back(
        *call(
            functools.partial(fine_kernel, plan),
            "fine",
            pieces,
            (band, fine_scale, *region, *fine_weights),
            smem=2,
        )
    )
    partner_cot = swapped(coarse_cotangent)
    own, grouped = call(
        functools.partial(merge_kernel, plan),
        "merge",
        [
            jax.ShapeDtypeStruct((plan.merged, width2), BF16),
            jax.ShapeDtypeStruct((plan.merged, 4 * width), BF16),
        ],
        (*fine_result, group, merge_gain, merge_weight),
    )
    partner = swapped(own)
    coarse_output, *grads = call(
        functools.partial(coarse_kernel, plan),
        "coarse",
        [jax.ShapeDtypeStruct(coarse_cotangent.shape, BF16)] + pieces,
        (
            coarse_scale,
            own,
            partner,
            coarse_cotangent,
            partner_cot,
            grouped,
            coarse_inward,
            coarse_outward,
            coarse_gain,
            merge_gain,
            merge_weight,
            ungroup,
        ),
        smem=1,
        scratch=[
            pltpu.VMEM((2 * plan.merged, width2), F32),
            pltpu.VMEM((plan.merged, width2), F32),
        ],
    )
    grads = gather(*grads)
    token_pieces = give_back(
        *call(
            functools.partial(fine_back_kernel, plan),
            "fine_back",
            pieces,
            (band, fine_scale, *region, *grads, *fine_weights),
            smem=2,
        )
    )
    (token_grad,) = call(
        functools.partial(unpack_kernel, plan),
        "unpack",
        [jax.ShapeDtypeStruct(tokens.shape, BF16)],
        (*token_pieces, unpack),
        keep_out=False,
    )
    return (coarse_output, token_grad)


def solution(mesh):
    whole, cells = P(), P(None, "lat", "lon", None)
    return jax.shard_map(
        local,
        mesh=mesh,
        in_specs=(cells, P("lat", "lon")) + (whole,) * 11 + (cells,),
        out_specs=(cells, cells),
        check_vma=False,
    )
```

```python
import functools

import jax
import jax.numpy as jnp
import numpy as np
from jax import lax
from jax.experimental import pallas as pl
from jax.experimental.pallas import tpu as pltpu
from jax.sharding import PartitionSpec as P

HEADS = 4
HEADS2 = 8
WIN_LAT = 6
WIN_LON = 12

EPS_NORM = 1e-05
EPS_HEAD = 1e-06

F32 = jnp.float32
BF16 = jnp.bfloat16


def shifted_to(x, by_lat, by_lon):
    lats, lons = lax.axis_size("lat"), lax.axis_size("lon")
    pairs = [
        (i * lons + j, ((i + by_lat) % lats) * lons + (j + by_lon) % lons)
        for i in range(lats)
        for j in range(lons)
    ]
    return lax.ppermute(x, ("lat", "lon"), pairs)


def swapped(x):
    return lax.ppermute(x, "lat", [(i, i ^ 1) for i in range(lax.axis_size("lat"))])


def up8(n):
    return -(-n // 8) * 8


class Plan:
    def __init__(self, levels, height, breadth):
        half_lat, half_lon = WIN_LAT // 2, WIN_LON // 2
        assert height == WIN_LAT and breadth % WIN_LON == 0
        self.levels, self.height, self.breadth = levels, height, breadth
        self.cells = levels * height * breadth
        windows = breadth // WIN_LON
        cols = [(0, half_lon)]
        for w in range(1, windows):
            cols.append((half_lon + (w - 1) * WIN_LON, half_lon + w * WIN_LON))
        edge = [(breadth - half_lon, breadth)]

        def piece(first_row, ranges):
            rows, spans = [], []
            for low, high in ranges:
                cells = [
                    (l * height + r) * breadth + c
                    for l in range(levels)
                    for r in range(first_row, first_row + half_lat)
                    for c in range(low, high)
                ]
                spans.append((len(rows), up8(len(cells)), len(cells)))
                rows += cells + [-1] * (up8(len(cells)) - len(cells))
            return rows, spans

        a_rows, self.a_spans = piece(0, cols)
        b_rows, _ = piece(half_lat, cols)
        c_rows, self.c_spans = piece(0, edge)
        d_rows, _ = piece(half_lat, edge)
        self.sizes = [len(a_rows), len(b_rows), len(c_rows), len(d_rows)]
        order = np.array(a_rows + b_rows + c_rows + d_rows)
        self.rows = len(order)
        self.pack = (order[:, None] == np.arange(self.cells)[None, :]).astype(np.float32)
        half_h, half_b = height // 2, breadth // 2
        group = [
            (l * height + 2 * r + i) * breadth + 2 * c + j
            for j in range(2)
            for i in range(2)
            for l in range(levels)
            for r in range(half_h)
            for c in range(half_b)
        ]
        natural = (np.array(group)[:, None] == np.arange(self.cells)[None, :]).astype(np.float32)
        self.group = natural @ self.pack.T
        self.merged = levels * half_h * half_b
        self.masks = []
        for w in range(windows):
            size, real = self.a_spans[w][1], self.a_spans[w][2]
            block = np.where(np.arange(size) < real, 0, 2)
            upper = np.where(np.arange(size) < real, 1, 2)
            marks = [block, upper] + ([block, upper] if w == 0 else [])
            marks = np.concatenate(marks)
            flat = np.minimum(marks, 1) * (marks == 2)
            apart = (marks[:, None] == marks[None, :]).astype(np.float32)
            whole = (flat[:, None] == flat[None, :]).astype(np.float32)
            self.masks.append(np.stack([apart, whole]))

    def window_rows(self, w, a, b, c=None, d=None):
        start, size, _ = self.a_spans[w]
        parts = [x[...].astype(F32)[start : start + size] for x in (a, b)]
        if w == 0:
            parts += [x[...].astype(F32) for x in (c, d)]
        return jnp.concatenate(parts, axis=0)

    def length(self, w):
        return self.masks[w].shape[-1]

    def put_pieces(self, outs, first, others):
        a, b = [], []
        for w, (_, size, _) in enumerate(self.a_spans):
            rows = first if w == 0 else others[w - 1][...].astype(F32)
            a.append(rows[:size])
            b.append(rows[size : 2 * size])
        base = 2 * self.a_spans[0][1]
        edge = self.c_spans[0][1]
        values = (
            jnp.concatenate(a, axis=0),
            jnp.concatenate(b, axis=0),
            first[base : base + edge],
            first[base + edge :],
        )
        for out, value in zip(outs, values):
            out[...] = value.astype(BF16)


def mm(a, b):
    return lax.dot_general(a, b, (((1,), (0,)), ((), ())), preferred_element_type=F32)


def mm_t(a, b):
    return lax.dot_general(a, b, (((1,), (1,)), ((), ())), preferred_element_type=F32)


def t_mm(a, b):
    return lax.dot_general(a, b, (((0,), (0,)), ((), ())), preferred_element_type=F32)


def norm_parts(values):
    average = jnp.mean(values, axis=-1, keepdims=True)
    centred = values - average
    spread = jnp.mean(centred * centred, axis=-1, keepdims=True)
    factor = lax.rsqrt(spread + EPS_NORM)
    return centred * factor, factor


def norm_back(unit, factor, grad):
    first = jnp.mean(grad, axis=-1, keepdims=True)
    second = jnp.mean(grad * unit, axis=-1, keepdims=True)
    return factor * (grad - first - unit * second)


def head_lanes(lanes, size, index):
    lane = lax.broadcasted_iota(jnp.int32, (1, lanes), 1)
    return (lane >= index * size) & (lane < (index + 1) * size)


def head_mean_matrix(lanes, size):
    row = lax.broadcasted_iota(jnp.int32, (lanes, lanes), 0)
    col = lax.broadcasted_iota(jnp.int32, (lanes, lanes), 1)
    same = jnp.zeros((lanes, lanes), F32)
    for h in range(lanes // size):
        inside = (row >= h * size) & (row < (h + 1) * size) & (col >= h * size) & (col < (h + 1) * size)
        same = jnp.where(inside, 1.0 / size, same)
    return same.astype(BF16)


def unit_rows(rows, mean_matrix):
    squares = mm((rows * rows).astype(BF16), mean_matrix)
    factor = lax.rsqrt(squares + EPS_HEAD)
    return rows * factor, factor


def unit_back(unit, factor, grad, mean_matrix):
    overlap = mm((unit * grad).astype(BF16), mean_matrix)
    return factor * (grad - unit * overlap)


def spread_heads(rows, masks):
    return jnp.concatenate([jnp.where(m, rows, 0.0) for m in masks], axis=0).astype(BF16)


def join_heads(stacked, masks):
    n = stacked.shape[0] // len(masks)
    total = jnp.where(masks[0], stacked[:n], 0.0)
    for h in range(1, len(masks)):
        total = jnp.where(masks[h], stacked[h * n : (h + 1) * n], total)
    return total


def attend(query_stack, key_unit, values, masks, allowed):
    weights = jnp.exp(mm_t(query_stack, key_unit))
    if allowed is not None:
        weights = weights * jnp.concatenate([allowed] * len(masks), axis=0)
    totals = jnp.sum(weights, axis=-1, keepdims=True)
    probs = weights * (1.0 / totals)
    return probs


def attend_back(probs, query_stack, key_unit, values, mixture_grad, masks):
    grad_stack = spread_heads(mixture_grad, masks)
    probs_grad = mm_t(grad_stack, values)
    low = probs.astype(BF16)
    probs = probs.astype(F32)
    delta = jnp.sum(probs * probs_grad, axis=-1, keepdims=True)
    logits_grad = (probs * (probs_grad - delta)).astype(BF16)
    query_grad = join_heads(mm(logits_grad, key_unit), masks)
    key_grad = t_mm(logits_grad, query_stack)
    value_grad = t_mm(low, grad_stack)
    return query_grad, key_grad, value_grad


def bias_kernel(plan, tokens, land_sea, land_vector, pack, *outs):
    land = land_sea[...].astype(F32)
    breadth = plan.breadth
    eye = lax.broadcasted_iota(jnp.int32, (breadth, breadth), 0) == lax.broadcasted_iota(
        jnp.int32, (breadth, breadth), 1
    )
    vector = land_vector[...]
    rows = []
    for r in range(plan.height):
        column = jnp.sum(jnp.where(eye, land[r : r + 1, :], 0.0), axis=1, keepdims=True)
        rows.append(column * vector)
    biased = jnp.concatenate(
        [tokens[l, r].astype(F32) + rows[r] for l in range(plan.levels) for r in range(plan.height)],
        axis=0,
    ).astype(BF16)
    packed = mm(pack[...], biased)
    start = 0
    for out in outs:
        out[...] = packed[start : start + out.shape[0]].astype(BF16)
        start += out.shape[0]


def allowed_of(mask, first_band):
    return jnp.where(first_band, mask[0], mask[1])


def fine_window(rows, allowed, inward, outward, scale_lanes, masks, mean_matrix):
    inner = scale_lanes.shape[-1]
    packed = mm(rows.astype(BF16), inward).astype(BF16).astype(F32)
    query_unit, query_factor = unit_rows(packed[:, :inner], mean_matrix)
    key_unit, key_factor = unit_rows(packed[:, inner : 2 * inner], mean_matrix)
    values = packed[:, 2 * inner :].astype(BF16)
    query_stack = spread_heads(query_unit * scale_lanes, masks)
    probs = attend(query_stack, key_unit.astype(BF16), values, masks, allowed)
    mixture = join_heads(mm(probs.astype(BF16), values), masks).astype(BF16)
    unit, factor = norm_parts(mm(mixture, outward))
    return query_unit, query_factor, key_unit, key_factor, values, query_stack, probs, unit, factor


def scale_lanes_of(scales, masks, head_size):
    lanes = jnp.zeros(masks[0].shape, F32)
    for h, mask in enumerate(masks):
        lanes = jnp.where(mask, scales[h] / head_size, lanes)
    return lanes


def fine_setup(scales, inner):
    head_size = inner // HEADS
    masks = [head_lanes(inner, head_size, h) for h in range(HEADS)]
    return masks, scale_lanes_of(scales, masks, head_size), head_mean_matrix(inner, head_size)


def saved_shapes(n, inner, width):
    return [
        jax.ShapeDtypeStruct((n, inner), F32),
        jax.ShapeDtypeStruct((n, inner), F32),
        jax.ShapeDtypeStruct((n, inner), F32),
        jax.ShapeDtypeStruct((n, inner), F32),
        jax.ShapeDtypeStruct((n, inner), BF16),
        jax.ShapeDtypeStruct((HEADS * n, inner), BF16),
        jax.ShapeDtypeStruct((HEADS * n, n), BF16),
        jax.ShapeDtypeStruct((n, width), F32),
        jax.ShapeDtypeStruct((n, 1), F32),
    ]


SAVED = 9


def fine_kernel(plan, w, band, scales, inward, outward, gain, mask, *rest):
    pieces = rest[: 4 if w == 0 else 2]
    rest = rest[len(pieces) :]
    masks, scale_lanes, mean_matrix = fine_setup(scales, outward.shape[0])
    rows = plan.window_rows(w, *pieces)
    allowed = allowed_of(mask, band[0] == 0)
    saved = fine_window(rows, allowed, inward[...], outward[...], scale_lanes, masks, mean_matrix)
    result = rows + saved[-2] * gain[...]
    finish(plan, w, result, rest[:-SAVED])
    for out, value in zip(rest[-SAVED:], saved):
        out[...] = value.astype(out.dtype)


def finish(plan, w, result, refs):
    if w == 0:
        plan.put_pieces(refs[-4:], result, refs[:-4])
    else:
        refs[0][...] = result.astype(BF16)


def fine_back_kernel(plan, w, scales, inward, outward, gain, *rest):
    pieces = rest[: 4 if w == 0 else 2]
    saved = rest[len(pieces) : len(pieces) + SAVED]
    rest = rest[len(pieces) + SAVED :]
    masks, scale_lanes, mean_matrix = fine_setup(scales, outward.shape[0])
    query_unit, query_factor, key_unit, key_factor, values, query_stack, probs, unit, factor = (
        x[...] for x in saved
    )
    grad = plan.window_rows(w, *pieces)
    projected_grad = norm_back(unit, factor, grad * gain[...]).astype(BF16)
    mixture_grad = mm_t(projected_grad, outward[...])
    query_grad, key_grad, value_grad = attend_back(
        probs, query_stack, key_unit.astype(BF16), values, mixture_grad, masks
    )
    query_grad = unit_back(query_unit, query_factor, query_grad * scale_lanes, mean_matrix)
    key_grad = unit_back(key_unit, key_factor, key_grad, mean_matrix)
    packed_grad = jnp.concatenate(
        [query_grad.astype(BF16), key_grad.astype(BF16), value_grad.astype(BF16)], axis=1
    )
    finish(plan, w, grad + mm_t(packed_grad, inward[...]), rest)


def merge_kernel(plan, a, b, c, d, group, gain, weight, coarse, grouped_out):
    pieces = jnp.concatenate([x[...].astype(F32) for x in (a, b, c, d)], axis=0).astype(BF16)
    rows = mm(group[...], pieces)
    n = plan.merged
    grouped = jnp.concatenate([rows[g * n : (g + 1) * n] for g in range(4)], axis=1)
    unit, _ = norm_parts(grouped)
    normed = (unit * gain[...]).astype(BF16)
    coarse[...] = mm(normed, weight[...]).astype(BF16)
    grouped_out[...] = grouped.astype(BF16)


def coarse_kernel(
    plan,
    scales,
    own,
    partner,
    own_cot,
    partner_cot,
    grouped,
    inward,
    outward,
    gain,
    merge_gain,
    merge_weight,
    ungroup,
    coarse_out,
    ga,
    gb,
    gc,
    gd,
    cot_rows,
    out_rows,
):
    inner = outward.shape[0]
    head_size = inner // HEADS2
    n = plan.merged
    half_b = plan.breadth // 2
    lines = [(l, r) for l in range(plan.levels) for r in range(plan.height // 2)]
    for k, (l, r) in enumerate(lines):
        cot_rows[k * half_b : (k + 1) * half_b, :] = own_cot[l, r].astype(F32)
        cot_rows[n + k * half_b : n + (k + 1) * half_b, :] = partner_cot[l, r].astype(F32)
    rows = jnp.concatenate([own[...].astype(F32), partner[...].astype(F32)], axis=0)
    packed = mm(rows.astype(BF16), inward[...]).astype(BF16).astype(F32)
    part = 256 if inner % 256 == 0 else inner
    per = part // head_size
    masks = [head_lanes(part, head_size, h) for h in range(per)]
    mean_matrix = head_mean_matrix(part, head_size)
    saved, mixtures = [], []
    for g in range(inner // part):
        low = g * part
        scale_lanes = scale_lanes_of([scales[g * per + h] for h in range(per)], masks, head_size)
        query_unit, query_factor = unit_rows(packed[:, low : low + part], mean_matrix)
        key_unit, key_factor = unit_rows(packed[:, inner + low : inner + low + part], mean_matrix)
        values = packed[:, 2 * inner + low : 2 * inner + low + part].astype(BF16)
        query_stack = spread_heads(query_unit * scale_lanes, masks)
        key_low = key_unit.astype(BF16)
        probs = attend(query_stack, key_low, values, masks, None)
        mixtures.append(join_heads(mm(probs.astype(BF16), values), masks).astype(BF16))
        saved.append(
            (query_unit, query_factor, key_unit, key_factor, values, query_stack, key_low, probs, scale_lanes)
        )
    unit, factor = norm_parts(mm(jnp.concatenate(mixtures, axis=1), outward[...]))
    out_rows[...] = rows[:n] + unit[:n] * gain[...]
    for k, (l, r) in enumerate(lines):
        coarse_out[l, r] = out_rows[k * half_b : (k + 1) * half_b, :].astype(BF16)

    cot = cot_rows[...]
    projected_grad = norm_back(unit, factor, cot * gain[...]).astype(BF16)
    mixture_grad = mm_t(projected_grad, outward[...])
    query_grads, key_grads, value_grads = [], [], []
    for g, (query_unit, query_factor, key_unit, key_factor, values, query_stack, key_low, probs, scale_lanes) in enumerate(saved):
        low = g * part
        query_grad, key_grad, value_grad = attend_back(
            probs, query_stack, key_low, values, mixture_grad[:, low : low + part], masks
        )
        query_grads.append(
            unit_back(query_unit[:n], query_factor[:n], query_grad[:n] * scale_lanes, mean_matrix).astype(BF16)
        )
        key_grads.append(unit_back(key_unit[:n], key_factor[:n], key_grad[:n], mean_matrix).astype(BF16))
        value_grads.append(value_grad[:n].astype(BF16))
    packed_grad = jnp.concatenate(query_grads + key_grads + value_grads, axis=1)
    coarse_grad = (cot[:n] + mm_t(packed_grad, inward[...])).astype(BF16)

    normed_grad = mm_t(coarse_grad, merge_weight[...])
    merge_unit, merge_factor = norm_parts(grouped[...].astype(F32))
    grouped_grad = norm_back(merge_unit, merge_factor, normed_grad * merge_gain[...])
    width = grouped_grad.shape[1] // 4
    stacked = jnp.concatenate(
        [grouped_grad[:, g * width : (g + 1) * width] for g in range(4)], axis=0
    ).astype(BF16)
    pieces = mm(ungroup[...], stacked)
    start = 0
    for out in (ga, gb, gc, gd):
        out[...] = pieces[start : start + out.shape[0]].astype(BF16)
        start += out.shape[0]


def unpack_kernel(plan, a, b, c, d, unpack, out):
    pieces = jnp.concatenate([x[...].astype(F32) for x in (a, b, c, d)], axis=0).astype(BF16)
    rows = mm(unpack[...], pieces)
    k = 0
    for l in range(plan.levels):
        for r in range(plan.height):
            out[l, r] = rows[k : k + plan.breadth].astype(BF16)
            k += plan.breadth


SMEM = functools.partial(pl.BlockSpec, memory_space=pltpu.SMEM)
VMEM = functools.partial(pl.BlockSpec, memory_space=pltpu.VMEM)


def call(kernel, name, outs, args, smem=0, scratch=(), keep_in=True, keep_out=True, cost=None):
    specs = [SMEM()] * smem + [VMEM()] * (len(args) - smem)
    space = pltpu.VMEM if keep_in else pltpu.HBM
    near = tuple(pltpu.with_memory_space_constraint(x, space) for x in args[smem:])
    args = tuple(args[:smem]) + near
    if keep_out:
        outs = [pltpu.VMEM(o.shape, o.dtype) for o in outs]
    return pl.pallas_call(
        kernel,
        name=name,
        out_shape=outs,
        in_specs=specs,
        out_specs=[VMEM() for _ in outs],
        scratch_shapes=scratch,
        cost_estimate=cost,
        compiler_params=pltpu.CompilerParams(vmem_limit_bytes=24 * 1024 * 1024),
    )(*args)


def load_kernel(after, *refs):
    n = (len(refs) - 1) // 2
    sems = refs[-1]
    copies = [pltpu.make_async_copy(refs[k], refs[n + k], sems.at[k]) for k in range(n)]
    for copy in copies:
        copy.start()
    for copy in copies:
        copy.wait()


def load(after, args):
    anywhere = pl.BlockSpec(memory_space=pl.ANY)
    args = tuple(pltpu.with_memory_space_constraint(x, pltpu.HBM) for x in args)
    return pl.pallas_call(
        load_kernel,
        name="load",
        out_shape=[pltpu.VMEM(x.shape, x.dtype) for x in args],
        in_specs=[anywhere] * (len(args) + 1),
        out_specs=[VMEM() for _ in args],
        scratch_shapes=[pltpu.SemaphoreType.DMA((len(args),))],
        compiler_params=pltpu.CompilerParams(vmem_limit_bytes=24 * 1024 * 1024),
    )(after, *args)


def local(
    tokens,
    land_sea,
    land_vector,
    fine_inward,
    fine_outward,
    fine_gain,
    fine_scale,
    merge_gain,
    merge_weight,
    coarse_inward,
    coarse_outward,
    coarse_gain,
    coarse_scale,
    coarse_cotangent,
):
    levels, height, breadth, width = tokens.shape
    width2 = coarse_cotangent.shape[-1]
    plan = Plan(levels, height, breadth)
    pieces = [jax.ShapeDtypeStruct((n, width), BF16) for n in plan.sizes]
    constant = lambda x: jnp.asarray(x, BF16)
    row = lambda x: x.reshape(1, -1)
    band = lax.axis_index("lat").astype(jnp.int32).reshape(1)
    masks = [jnp.asarray(m, F32) for m in plan.masks]

    def gather(a, b, c, d):
        return a, shifted_to(b, 1, 0), shifted_to(c, 0, 1), shifted_to(d, 1, 1)

    def give_back(a, b, c, d):
        return a, shifted_to(b, -1, 0), shifted_to(c, 0, -1), shifted_to(d, -1, -1)

    biased = call(
        functools.partial(bias_kernel, plan),
        "bias",
        pieces,
        (tokens, land_sea, row(land_vector), constant(plan.pack)),
        keep_in=False,
    )
    region = gather(*biased)
    fine_inward, fine_outward, fine_gain, group, merge_gain, *masks = load(
        biased[0],
        (fine_inward, fine_outward, row(fine_gain), constant(plan.group), row(merge_gain), *masks),
    )
    fine_weights = (fine_inward, fine_outward, fine_gain)
    cost = pl.CostEstimate(flops=2 * 10**8, transcendentals=0, bytes_accessed=10**6)
    windows = len(plan.masks)
    inner = fine_outward.shape[0]
    shapes = [
        [jax.ShapeDtypeStruct((plan.length(w), width), BF16)]
        + saved_shapes(plan.length(w), inner, width)
        for w in range(windows)
    ]
    others, saved = [], [None] * windows
    for w in range(1, windows):
        result, *saved[w] = call(
            functools.partial(fine_kernel, plan, w),
            "fine_inside",
            shapes[w],
            (band, fine_scale, *fine_weights, masks[w], region[0], region[1]),
            smem=2,
            cost=cost,
        )
        others.append(result)
    outs = call(
        functools.partial(fine_kernel, plan, 0),
        "fine_edge",
        pieces + shapes[0][1:],
        (band, fine_scale, *fine_weights, masks[0], *region, *others),
        smem=2,
        cost=cost,
    )
    saved[0] = outs[4:]
    merge_weight, coarse_inward, coarse_outward, coarse_gain, ungroup, unpack = load(
        outs[0],
        (
            merge_weight,
            coarse_inward,
            coarse_outward,
            row(coarse_gain),
            constant(plan.group.T),
            constant(plan.pack.T),
        ),
    )
    fine_result = give_back(*outs[:4])
    partner_cot = swapped(coarse_cotangent)
    own, grouped = call(
        functools.partial(merge_kernel, plan),
        "merge",
        [
            jax.ShapeDtypeStruct((plan.merged, width2), BF16),
            jax.ShapeDtypeStruct((plan.merged, 4 * width), BF16),
        ],
        (*fine_result, group, merge_gain, merge_weight),
    )
    partner = swapped(own)
    coarse_output, *grads = call(
        functools.partial(coarse_kernel, plan),
        "coarse",
        [jax.ShapeDtypeStruct(coarse_cotangent.shape, BF16)] + pieces,
        (
            coarse_scale,
            own,
            partner,
            coarse_cotangent,
            partner_cot,
            grouped,
            coarse_inward,
            coarse_outward,
            coarse_gain,
            merge_gain,
            merge_weight,
            ungroup,
        ),
        smem=1,
        scratch=[
            pltpu.VMEM((2 * plan.merged, width2), F32),
            pltpu.VMEM((plan.merged, width2), F32),
        ],
    )
    grads = gather(*grads)
    others = []
    for w in range(1, windows):
        (result,) = call(
            functools.partial(fine_back_kernel, plan, w),
            "fine_back_inside",
            shapes[w][:1],
            (fine_scale, *fine_weights, grads[0], grads[1], *saved[w]),
            smem=1,
            cost=cost,
        )
        others.append(result)
    token_pieces = give_back(
        *call(
            functools.partial(fine_back_kernel, plan, 0),
            "fine_back_edge",
            pieces,
            (fine_scale, *fine_weights, *grads, *saved[0], *others),
            smem=1,
            cost=cost,
        )
    )
    (token_grad,) = call(
        functools.partial(unpack_kernel, plan),
        "unpack",
        [jax.ShapeDtypeStruct(tokens.shape, BF16)],
        (*token_pieces, unpack),
        keep_out=False,
    )
    return (coarse_output, token_grad)


def solution(mesh):
    whole, cells = P(), P(None, "lat", "lon", None)
    return jax.shard_map(
        local,
        mesh=mesh,
        in_specs=(cells, P("lat", "lon")) + (whole,) * 11 + (cells,),
        out_specs=(cells, cells),
        check_vma=False,
    )
```

```python
import functools

import jax
import jax.numpy as jnp
import numpy as np
from jax import lax
from jax.experimental import pallas as pl
from jax.experimental.pallas import tpu as pltpu
from jax.sharding import PartitionSpec as P

HEADS = 4
HEADS2 = 8
WIN_LAT = 6
WIN_LON = 12

EPS_NORM = 1e-05
EPS_HEAD = 1e-06

F32 = jnp.float32
BF16 = jnp.bfloat16


def shifted_to(x, by_lat, by_lon):
    lats, lons = lax.axis_size("lat"), lax.axis_size("lon")
    pairs = [
        (i * lons + j, ((i + by_lat) % lats) * lons + (j + by_lon) % lons)
        for i in range(lats)
        for j in range(lons)
    ]
    return lax.ppermute(x, ("lat", "lon"), pairs)


def swapped(x):
    return lax.ppermute(x, "lat", [(i, i ^ 1) for i in range(lax.axis_size("lat"))])


def up8(n):
    return -(-n // 8) * 8


class Plan:
    def __init__(self, levels, height, breadth):
        half_lat, half_lon = WIN_LAT // 2, WIN_LON // 2
        assert height == WIN_LAT and breadth % WIN_LON == 0
        self.levels, self.height, self.breadth = levels, height, breadth
        self.cells = levels * height * breadth
        windows = breadth // WIN_LON
        cols = [(0, half_lon)]
        for w in range(1, windows):
            cols.append((half_lon + (w - 1) * WIN_LON, half_lon + w * WIN_LON))
        edge = [(breadth - half_lon, breadth)]

        def piece(first_row, ranges):
            rows, spans = [], []
            for low, high in ranges:
                cells = [
                    (l * height + r) * breadth + c
                    for l in range(levels)
                    for r in range(first_row, first_row + half_lat)
                    for c in range(low, high)
                ]
                spans.append((len(rows), up8(len(cells)), len(cells)))
                rows += cells + [-1] * (up8(len(cells)) - len(cells))
            return rows, spans

        a_rows, self.a_spans = piece(0, cols)
        b_rows, _ = piece(half_lat, cols)
        c_rows, self.c_spans = piece(0, edge)
        d_rows, _ = piece(half_lat, edge)
        self.sizes = [len(a_rows), len(b_rows), len(c_rows), len(d_rows)]
        order = np.array(a_rows + b_rows + c_rows + d_rows)
        self.rows = len(order)
        self.pack = (order[:, None] == np.arange(self.cells)[None, :]).astype(np.float32)
        half_h, half_b = height // 2, breadth // 2
        group = [
            (l * height + 2 * r + i) * breadth + 2 * c + j
            for j in range(2)
            for i in range(2)
            for l in range(levels)
            for r in range(half_h)
            for c in range(half_b)
        ]
        natural = (np.array(group)[:, None] == np.arange(self.cells)[None, :]).astype(np.float32)
        self.group = natural @ self.pack.T
        self.merged = levels * half_h * half_b
        self.masks = []
        for w in range(windows):
            size, real = self.a_spans[w][1], self.a_spans[w][2]
            block = np.where(np.arange(size) < real, 0, 2)
            upper = np.where(np.arange(size) < real, 1, 2)
            marks = [block, upper] + ([block, upper] if w == 0 else [])
            marks = np.concatenate(marks)
            flat = np.minimum(marks, 1) * (marks == 2)
            apart = (marks[:, None] == marks[None, :]).astype(np.float32)
            whole = (flat[:, None] == flat[None, :]).astype(np.float32)
            self.masks.append(np.stack([apart, whole]))

    def window_rows(self, w, a, b, c=None, d=None):
        start, size, _ = self.a_spans[w]
        parts = [x[...].astype(F32)[start : start + size] for x in (a, b)]
        if w == 0:
            parts += [x[...].astype(F32) for x in (c, d)]
        return jnp.concatenate(parts, axis=0)

    def length(self, w):
        return self.masks[w].shape[-1]

    def put_pieces(self, outs, first, others):
        a, b = [], []
        for w, (_, size, _) in enumerate(self.a_spans):
            rows = first if w == 0 else others[w - 1][...].astype(F32)
            a.append(rows[:size])
            b.append(rows[size : 2 * size])
        base = 2 * self.a_spans[0][1]
        edge = self.c_spans[0][1]
        values = (
            jnp.concatenate(a, axis=0),
            jnp.concatenate(b, axis=0),
            first[base : base + edge],
            first[base + edge :],
        )
        for out, value in zip(outs, values):
            out[...] = value.astype(BF16)


def mm(a, b):
    return lax.dot_general(a, b, (((1,), (0,)), ((), ())), preferred_element_type=F32)


def mm_t(a, b):
    return lax.dot_general(a, b, (((1,), (1,)), ((), ())), preferred_element_type=F32)


def t_mm(a, b):
    return lax.dot_general(a, b, (((0,), (0,)), ((), ())), preferred_element_type=F32)


def norm_parts(values):
    average = jnp.mean(values, axis=-1, keepdims=True)
    centred = values - average
    spread = jnp.mean(centred * centred, axis=-1, keepdims=True)
    factor = lax.rsqrt(spread + EPS_NORM)
    return centred * factor, factor


def norm_back(unit, factor, grad):
    first = jnp.mean(grad, axis=-1, keepdims=True)
    second = jnp.mean(grad * unit, axis=-1, keepdims=True)
    return factor * (grad - first - unit * second)


def head_lanes(lanes, size, index):
    lane = lax.broadcasted_iota(jnp.int32, (1, lanes), 1)
    return (lane >= index * size) & (lane < (index + 1) * size)


def head_mean_matrix(lanes, size):
    row = lax.broadcasted_iota(jnp.int32, (lanes, lanes), 0)
    col = lax.broadcasted_iota(jnp.int32, (lanes, lanes), 1)
    same = jnp.zeros((lanes, lanes), F32)
    for h in range(lanes // size):
        inside = (row >= h * size) & (row < (h + 1) * size) & (col >= h * size) & (col < (h + 1) * size)
        same = jnp.where(inside, 1.0 / size, same)
    return same.astype(BF16)


def unit_rows(rows, mean_matrix):
    squares = mm((rows * rows).astype(BF16), mean_matrix)
    factor = lax.rsqrt(squares + EPS_HEAD)
    return rows * factor, factor


def unit_back(unit, factor, grad, mean_matrix):
    overlap = mm((unit * grad).astype(BF16), mean_matrix)
    return factor * (grad - unit * overlap)


def spread_heads(rows, masks, blocks=1):
    n = rows.shape[0] // blocks
    return jnp.concatenate(
        [jnp.where(m, rows[b * n : (b + 1) * n], 0.0) for b in range(blocks) for m in masks], axis=0
    ).astype(BF16)


def join_heads(stacked, masks, blocks=1):
    heads = len(masks)
    n = stacked.shape[0] // (heads * blocks)
    parts = []
    for b in range(blocks):
        low = b * heads * n
        total = jnp.where(masks[0], stacked[low : low + n], 0.0)
        for h in range(1, heads):
            total = jnp.where(masks[h], stacked[low + h * n : low + (h + 1) * n], total)
        parts.append(total)
    return parts[0] if blocks == 1 else jnp.concatenate(parts, axis=0)


def attend(query_stack, key_unit, values, masks, allowed):
    weights = jnp.exp(mm_t(query_stack, key_unit))
    if allowed is not None:
        weights = weights * jnp.concatenate([allowed] * len(masks), axis=0)
    totals = jnp.sum(weights, axis=-1, keepdims=True)
    probs = weights * (1.0 / totals)
    return probs


def attend_back(probs, query_stack, key_unit, values, mixture_grad, masks, blocks=1):
    grad_stack = spread_heads(mixture_grad, masks, blocks)
    own = key_unit.shape[0] // blocks
    probs_grad = mm_t(grad_stack, values)
    low = probs.astype(BF16)
    probs = probs.astype(F32)
    delta = jnp.sum(probs * probs_grad, axis=-1, keepdims=True)
    logits_grad = (probs * (probs_grad - delta)).astype(BF16)
    query_grad = join_heads(mm(logits_grad[: own * len(masks)], key_unit), masks)
    key_grad = t_mm(logits_grad[:, :own], query_stack)
    value_grad = t_mm(low[:, :own], grad_stack)
    return query_grad, key_grad, value_grad


def bias_kernel(plan, tokens, land_sea, land_vector, pack, *outs):
    land = land_sea[...].astype(F32)
    breadth = plan.breadth
    eye = lax.broadcasted_iota(jnp.int32, (breadth, breadth), 0) == lax.broadcasted_iota(
        jnp.int32, (breadth, breadth), 1
    )
    vector = land_vector[...]
    rows = []
    for r in range(plan.height):
        column = jnp.sum(jnp.where(eye, land[r : r + 1, :], 0.0), axis=1, keepdims=True)
        rows.append(column * vector)
    biased = jnp.concatenate(
        [tokens[l, r].astype(F32) + rows[r] for l in range(plan.levels) for r in range(plan.height)],
        axis=0,
    ).astype(BF16)
    packed = mm(pack[...], biased)
    start = 0
    for out in outs:
        out[...] = packed[start : start + out.shape[0]].astype(BF16)
        start += out.shape[0]


def allowed_of(mask, first_band):
    return jnp.where(first_band, mask[0].astype(F32), mask[1].astype(F32))


def fine_window(rows, allowed, inward, outward, scale_lanes, masks, mean_matrix):
    inner = scale_lanes.shape[-1]
    packed = mm(rows.astype(BF16), inward).astype(BF16).astype(F32)
    query_unit, query_factor = unit_rows(packed[:, :inner], mean_matrix)
    key_unit, key_factor = unit_rows(packed[:, inner : 2 * inner], mean_matrix)
    values = packed[:, 2 * inner :].astype(BF16)
    query_stack = spread_heads(query_unit * scale_lanes, masks)
    probs = attend(query_stack, key_unit.astype(BF16), values, masks, allowed)
    mixture = join_heads(mm(probs.astype(BF16), values), masks).astype(BF16)
    unit, factor = norm_parts(mm(mixture, outward))
    return query_unit, query_factor, key_unit, key_factor, values, query_stack, probs, unit, factor


def scale_lanes_of(scales, masks, head_size):
    lanes = jnp.zeros(masks[0].shape, F32)
    for h, mask in enumerate(masks):
        lanes = jnp.where(mask, scales[:, h : h + 1] / head_size, lanes)
    return lanes


def fine_setup(scales, inner):
    head_size = inner // HEADS
    masks = [head_lanes(inner, head_size, h) for h in range(HEADS)]
    return masks, scale_lanes_of(scales[...], masks, head_size), head_mean_matrix(inner, head_size)


def saved_shapes(n, inner, width):
    return [
        jax.ShapeDtypeStruct((n, inner), F32),
        jax.ShapeDtypeStruct((n, inner), F32),
        jax.ShapeDtypeStruct((n, inner), F32),
        jax.ShapeDtypeStruct((n, inner), F32),
        jax.ShapeDtypeStruct((n, inner), BF16),
        jax.ShapeDtypeStruct((HEADS * n, inner), BF16),
        jax.ShapeDtypeStruct((HEADS * n, n), BF16),
        jax.ShapeDtypeStruct((n, width), F32),
        jax.ShapeDtypeStruct((n, 1), F32),
    ]


SAVED = 9


def fine_kernel(plan, w, band, inward, outward, gain, scales, mask, *rest):
    pieces = rest[: 4 if w == 0 else 2]
    rest = rest[len(pieces) :]
    masks, scale_lanes, mean_matrix = fine_setup(scales, outward.shape[0])
    rows = plan.window_rows(w, *pieces)
    allowed = allowed_of(mask, band[0] == 0)
    saved = fine_window(rows, allowed, inward[...], outward[...], scale_lanes, masks, mean_matrix)
    result = rows + saved[-2] * gain[...]
    finish(plan, w, result, rest[:-SAVED])
    for out, value in zip(rest[-SAVED:], saved):
        out[...] = value.astype(out.dtype)


def finish(plan, w, result, refs):
    if w == 0:
        plan.put_pieces(refs[-4:], result, refs[:-4])
    else:
        refs[0][...] = result.astype(BF16)


def fine_back_kernel(plan, w, inward_turned, outward_turned, gain, scales, *rest):
    pieces = rest[: 4 if w == 0 else 2]
    saved = rest[len(pieces) : len(pieces) + SAVED]
    rest = rest[len(pieces) + SAVED :]
    masks, scale_lanes, mean_matrix = fine_setup(scales, outward_turned.shape[1])
    query_unit, query_factor, key_unit, key_factor, values, query_stack, probs, unit, factor = (
        x[...] for x in saved
    )
    grad = plan.window_rows(w, *pieces)
    projected_grad = norm_back(unit, factor, grad * gain[...]).astype(BF16)
    mixture_grad = mm(projected_grad, outward_turned[...])
    query_grad, key_grad, value_grad = attend_back(
        probs, query_stack, key_unit.astype(BF16), values, mixture_grad, masks
    )
    query_grad = unit_back(query_unit, query_factor, query_grad * scale_lanes, mean_matrix)
    key_grad = unit_back(key_unit, key_factor, key_grad, mean_matrix)
    packed_grad = jnp.concatenate(
        [query_grad.astype(BF16), key_grad.astype(BF16), value_grad.astype(BF16)], axis=1
    )
    finish(plan, w, grad + mm(packed_grad, inward_turned[...]), rest)


def merge_kernel(plan, a, b, c, d, group, gain, weight, after, coarse, unit_out, factor_out):
    pieces = jnp.concatenate([x[...].astype(F32) for x in (a, b, c, d)], axis=0).astype(BF16)
    rows = mm(group[...], pieces)
    n = plan.merged
    grouped = jnp.concatenate([rows[g * n : (g + 1) * n] for g in range(4)], axis=1)
    unit, factor = norm_parts(grouped)
    normed = (unit * gain[...]).astype(BF16)
    coarse[...] = mm(normed, weight[...]).astype(BF16)
    unit_out[...] = unit
    factor_out[...] = factor


def cotangent_kernel(plan, own_cot, partner_cot, gain, rows_out, scaled_out, mean_out):
    n = plan.merged
    half_b = plan.breadth // 2
    lines = [(l, r) for l in range(plan.levels) for r in range(plan.height // 2)]
    for k, (l, r) in enumerate(lines):
        for start, cot in ((0, own_cot), (n, partner_cot)):
            low = start + k * half_b
            rows_out[low : low + half_b, :] = cot[l, r].astype(F32)
    scaled = rows_out[...] * gain[...]
    scaled_out[...] = scaled
    mean_out[...] = jnp.mean(scaled, axis=-1, keepdims=True)


def output_kernel(plan, rows, coarse_out, scratch):
    half_b = plan.breadth // 2
    scratch[...] = rows[...].astype(F32)
    lines = [(l, r) for l in range(plan.levels) for r in range(plan.height // 2)]
    for k, (l, r) in enumerate(lines):
        coarse_out[l, r] = scratch[k * half_b : (k + 1) * half_b, :].astype(BF16)


def coarse_kernel(
    plan,
    scales,
    own,
    partner,
    cot,
    scaled_cot,
    cot_mean,
    merge_unit,
    merge_factor,
    inward,
    outward,
    inward_turned,
    outward_turned,
    gain,
    merge_gain,
    merge_turned,
    ungroup,
    coarse_out,
    ga,
    gb,
    gc,
    gd,
):
    inner = outward.shape[0]
    head_size = inner // HEADS2
    n = plan.merged
    rows = jnp.concatenate([own[...].astype(F32), partner[...].astype(F32)], axis=0)
    packed = mm(rows.astype(BF16), inward[...]).astype(BF16).astype(F32)
    part = 256 if inner % 256 == 0 else inner
    per = part // head_size
    masks = [head_lanes(part, head_size, h) for h in range(per)]
    mean_matrix = head_mean_matrix(part, head_size)
    saved, mixtures = [], []
    for g in range(inner // part):
        low = g * part
        scale_lanes = scale_lanes_of(scales[:, g * per : (g + 1) * per], masks, head_size)
        query_unit, query_factor = unit_rows(packed[:, low : low + part], mean_matrix)
        key_unit, key_factor = unit_rows(packed[:, inner + low : inner + low + part], mean_matrix)
        values = packed[:, 2 * inner + low : 2 * inner + low + part].astype(BF16)
        query_stack = spread_heads(query_unit * scale_lanes, masks, 2)
        key_low = key_unit.astype(BF16)
        probs = attend(query_stack, key_low, values, masks, None)
        mixtures.append(join_heads(mm(probs.astype(BF16), values), masks, 2).astype(BF16))
        saved.append(
            (query_unit, query_factor, key_unit, key_factor, values, query_stack, key_low, probs, scale_lanes)
        )
    unit, factor = norm_parts(mm(jnp.concatenate(mixtures, axis=1), outward[...]))
    coarse_out[...] = (rows[:n] + unit[:n] * gain[...]).astype(BF16)

    grad = scaled_cot[...]
    second = jnp.mean(grad * unit, axis=-1, keepdims=True)
    projected_grad = (factor * (grad - cot_mean[...] - unit * second)).astype(BF16)
    mixture_grad = mm(projected_grad, outward_turned[...])
    query_grads, key_grads, value_grads = [], [], []
    for g, (query_unit, query_factor, key_unit, key_factor, values, query_stack, key_low, probs, scale_lanes) in enumerate(saved):
        low = g * part
        query_grad, key_grad, value_grad = attend_back(
            probs, query_stack, key_low, values, mixture_grad[:, low : low + part], masks, 2
        )
        query_grads.append(
            unit_back(query_unit[:n], query_factor[:n], query_grad * scale_lanes, mean_matrix).astype(BF16)
        )
        key_grads.append(unit_back(key_unit[:n], key_factor[:n], key_grad, mean_matrix).astype(BF16))
        value_grads.append(value_grad.astype(BF16))
    packed_grad = jnp.concatenate(query_grads + key_grads + value_grads, axis=1)
    coarse_grad = (cot[:n] + mm(packed_grad, inward_turned[...])).astype(BF16)

    normed_grad = mm(coarse_grad, merge_turned[...])
    grouped_grad = norm_back(merge_unit[...], merge_factor[...], normed_grad * merge_gain[...])
    width = grouped_grad.shape[1] // 4
    stacked = jnp.concatenate(
        [grouped_grad[:, g * width : (g + 1) * width] for g in range(4)], axis=0
    ).astype(BF16)
    pieces = mm(ungroup[...], stacked)
    start = 0
    for out in (ga, gb, gc, gd):
        out[...] = pieces[start : start + out.shape[0]].astype(BF16)
        start += out.shape[0]


def unpack_kernel(plan, a, b, c, d, unpack, out):
    pieces = jnp.concatenate([x[...].astype(F32) for x in (a, b, c, d)], axis=0).astype(BF16)
    rows = mm(unpack[...], pieces)
    k = 0
    for l in range(plan.levels):
        for r in range(plan.height):
            out[l, r] = rows[k : k + plan.breadth].astype(BF16)
            k += plan.breadth


SMEM = functools.partial(pl.BlockSpec, memory_space=pltpu.SMEM)
VMEM = functools.partial(pl.BlockSpec, memory_space=pltpu.VMEM)


def call(kernel, name, outs, args, smem=0, scratch=(), keep_in=True, keep_out=True, cost=None, loads=()):
    n_in, n_out, n_loads = len(args), len(outs), len(loads)
    space = pltpu.VMEM if keep_in else pltpu.HBM
    near = tuple(pltpu.with_memory_space_constraint(x, space) for x in args[smem:])
    far = tuple(pltpu.with_memory_space_constraint(x, pltpu.HBM) for x in loads)
    if keep_out:
        outs = [pltpu.VMEM(o.shape, o.dtype) for o in outs]

    def body(*refs):
        ins, refs = refs[:n_in], refs[n_in:]
        sources, refs = refs[:n_loads], refs[n_loads:]
        results, refs = refs[:n_out], refs[n_out:]
        targets, rest = refs[:n_loads], refs[n_loads:]
        copies = []
        if n_loads:
            *rest, sems = rest
            copies = [
                pltpu.make_async_copy(x, y, sems.at[k]) for k, (x, y) in enumerate(zip(sources, targets))
            ]
        for copy in copies:
            copy.start()
        kernel(*ins, *results, *rest)
        for copy in copies:
            copy.wait()

    anywhere = pl.BlockSpec(memory_space=pl.ANY)
    return pl.pallas_call(
        body,
        name=name,
        out_shape=outs + [pltpu.VMEM(x.shape, x.dtype) for x in loads],
        in_specs=[SMEM()] * smem + [VMEM()] * (n_in - smem) + [anywhere] * n_loads,
        out_specs=[VMEM()] * (n_out + n_loads),
        scratch_shapes=list(scratch) + ([pltpu.SemaphoreType.DMA((n_loads,))] if n_loads else []),
        cost_estimate=cost,
        compiler_params=pltpu.CompilerParams(vmem_limit_bytes=20 * 1024 * 1024),
    )(*args[:smem], *near, *far)


def turn(source, target):
    step = 256 if source.shape[0] % 256 == 0 else source.shape[0]
    for k in range(0, source.shape[0], step):
        target[:, k : k + step] = source[k : k + step, :].T


def turn_kernel(*refs):
    half = len(refs) // 2
    for source, target in zip(refs[:half], refs[half:]):
        turn(source, target)
    if len(refs) % 2:
        refs[-1][...] = jnp.zeros(refs[-1].shape, refs[-1].dtype)


def local(
    tokens,
    land_sea,
    land_vector,
    fine_inward,
    fine_outward,
    fine_gain,
    fine_scale,
    merge_gain,
    merge_weight,
    coarse_inward,
    coarse_outward,
    coarse_gain,
    coarse_scale,
    coarse_cotangent,
):
    levels, height, breadth, width = tokens.shape
    width2 = coarse_cotangent.shape[-1]
    plan = Plan(levels, height, breadth)
    pieces = [jax.ShapeDtypeStruct((n, width), BF16) for n in plan.sizes]
    constant = lambda x: jnp.asarray(x, BF16)
    row = lambda x: x.reshape(1, -1)
    band = lax.axis_index("lat").astype(jnp.int32).reshape(1)
    masks = [constant(m) for m in plan.masks]

    def gather(a, b, c, d):
        return a, shifted_to(b, 1, 0), shifted_to(c, 0, 1), shifted_to(d, 1, 1)

    def give_back(a, b, c, d):
        return a, shifted_to(b, -1, 0), shifted_to(c, 0, -1), shifted_to(d, -1, -1)

    biased = call(
        functools.partial(bias_kernel, plan),
        "bias",
        pieces,
        (tokens, land_sea, row(land_vector), constant(plan.pack)),
        keep_in=False,
    )
    region = gather(*biased)
    (
        fine_inward,
        fine_outward,
        fine_gain,
        fine_scale,
        coarse_scale,
        merge_gain,
        coarse_gain,
        *masks,
    ) = call(
        lambda after: None,
        "load",
        [],
        (biased[0],),
        loads=(
            fine_inward,
            fine_outward,
            row(fine_gain),
            row(fine_scale),
            row(coarse_scale),
            row(merge_gain),
            row(coarse_gain),
            *masks,
        ),
    )
    cost = pl.CostEstimate(flops=2 * 10**8, transcendentals=0, bytes_accessed=10**6)
    windows = len(plan.masks)
    inner = fine_outward.shape[0]
    shapes = [
        [jax.ShapeDtypeStruct((plan.length(w), width), BF16)]
        + saved_shapes(plan.length(w), inner, width)
        for w in range(windows)
    ]
    fine_weights = (fine_inward, fine_outward, fine_gain, fine_scale)
    others, saved = [], [None] * windows
    for w in range(1, windows):
        first = w == 1
        result, *saved[w] = call(
            functools.partial(fine_kernel, plan, w),
            "fine_inside",
            shapes[w],
            (band, *fine_weights, masks[w], region[0], region[1]),
            smem=1,
            cost=cost,
            loads=(coarse_inward,) if first else (),
        )
        if first:
            (coarse_inward,) = saved[w][SAVED:]
            del saved[w][SAVED:]
        others.append(result)
    outs = call(
        functools.partial(fine_kernel, plan, 0),
        "fine_edge",
        pieces + shapes[0][1:],
        (band, *fine_weights, masks[0], *region, *others),
        smem=1,
        cost=cost,
    )
    saved[0] = outs[4:]
    fine_result = give_back(*outs[:4])
    large = (coarse_inward, merge_weight)
    coarse_inward_turned, merge_turned, done = call(
        turn_kernel,
        "turn_large",
        [jax.ShapeDtypeStruct(x.shape[::-1], x.dtype) for x in large]
        + [jax.ShapeDtypeStruct((8, 128), F32)],
        large,
        cost=cost,
    )
    partner_cot = swapped(coarse_cotangent)
    cot, scaled_cot, cot_mean = call(
        functools.partial(cotangent_kernel, plan),
        "cotangent",
        [
            jax.ShapeDtypeStruct((2 * plan.merged, width2), F32),
            jax.ShapeDtypeStruct((2 * plan.merged, width2), F32),
            jax.ShapeDtypeStruct((2 * plan.merged, 1), F32),
        ],
        (coarse_cotangent, partner_cot, coarse_gain),
    )
    own, merge_unit, merge_factor = call(
        functools.partial(merge_kernel, plan),
        "merge",
        [
            jax.ShapeDtypeStruct((plan.merged, width2), BF16),
            jax.ShapeDtypeStruct((plan.merged, 4 * width), F32),
            jax.ShapeDtypeStruct((plan.merged, 1), F32),
        ],
        (*fine_result, constant(plan.group), merge_gain, merge_weight, done),
    )
    turned = (fine_inward, fine_outward, coarse_outward)
    fine_inward_turned, fine_outward_turned, coarse_outward_turned = call(
        turn_kernel,
        "turn_small",
        [jax.ShapeDtypeStruct(x.shape[::-1], x.dtype) for x in turned],
        turned,
        cost=cost,
    )
    partner = swapped(own)
    output_rows, *grads = call(
        functools.partial(coarse_kernel, plan),
        "coarse",
        [jax.ShapeDtypeStruct((plan.merged, width2), BF16)] + pieces,
        (
            coarse_scale,
            own,
            partner,
            cot,
            scaled_cot,
            cot_mean,
            merge_unit,
            merge_factor,
            coarse_inward,
            coarse_outward,
            coarse_inward_turned,
            coarse_outward_turned,
            coarse_gain,
            merge_gain,
            merge_turned,
            constant(plan.group.T),
        ),
    )
    (coarse_output,) = call(
        functools.partial(output_kernel, plan),
        "output",
        [jax.ShapeDtypeStruct(coarse_cotangent.shape, BF16)],
        (output_rows,),
        scratch=[pltpu.VMEM(output_rows.shape, F32)],
    )
    grads = gather(*grads)
    back_weights = (fine_inward_turned, fine_outward_turned, fine_gain, fine_scale)
    others = []
    for w in range(1, windows):
        (result,) = call(
            functools.partial(fine_back_kernel, plan, w),
            "fine_back_inside",
            shapes[w][:1],
            (*back_weights, grads[0], grads[1], *saved[w]),
            cost=cost,
        )
        others.append(result)
    token_pieces = give_back(
        *call(
            functools.partial(fine_back_kernel, plan, 0),
            "fine_back_edge",
            pieces,
            (*back_weights, *grads, *saved[0], *others),
            cost=cost,
        )
    )
    (token_grad,) = call(
        functools.partial(unpack_kernel, plan),
        "unpack",
        [jax.ShapeDtypeStruct(tokens.shape, BF16)],
        (*token_pieces, constant(plan.pack.T)),
        keep_out=False,
    )
    return (coarse_output, token_grad)


def solution(mesh):
    whole, cells = P(), P(None, "lat", "lon", None)
    return jax.shard_map(
        local,
        mesh=mesh,
        in_specs=(cells, P("lat", "lon")) + (whole,) * 11 + (cells,),
        out_specs=(cells, cells),
        check_vma=False,
    )
```
